32 devices in a mesh: section: 4 (over y, x), row: 8 (over z, core).
Axes of the slice: x: 2, y: 2, z: 4, core: 2. Of those that a mesh axis runs over, the one named last changes fastest.
Arguments:
- omega: bfloat16 [2048, 8192], P('section', 'row'), may hold values from -0.5 to 0.5
- basis: bfloat16 [8192, 1024], P('row', 'section'), may hold values from -6 to 6
- vectors: bfloat16 [4, 8192], P(None, 'row'), may hold values from -6 to 6
Outputs:
- ortho: float32 [4, 8192], P(None, ('row', 'section'))
- coeffs: float32 [4, 1024], P(None, 'section')
The draws below stay inside these ranges and needn't reach their ends.
All inputs are finite; a program needn't handle non-finite values.
Results may differ from the reference program's by a relative error of at most 0.0021.
Values may be sent and summed in bfloat16 or wider, within the bound.
A program may use at most 64 MiB of HBM per device.

```python
import jax
import jax.numpy as jnp
from jax import lax

BLOCK = 256
NVEC = 4
SKETCH = 2048
NROWS = 8192
COLUMNS = 1024
N_SECTION = 4


def block_levels(own_key, extent, split, least, largest):
    gain = 1.0
    for position, parts in split:
        draws = jax.random.uniform(jax.random.fold_in(jax.random.fold_in(own_key, 6), position), (parts,), jnp.float32, least / len(split), largest / len(split))
        gain = gain * jnp.repeat(jnp.exp(draws), extent[position] // parts).reshape((-1,) + (1,) * (len(extent) - 1 - position))
    return gain


def centred(own_key, extent, width, bound, shards=(), dtype=jnp.bfloat16):
    result = width * jax.random.normal(own_key, extent, jnp.float32)
    if shards:
        result = result * block_levels(own_key, extent, shards, -0.22, 0.18)
    return jnp.clip(result, -bound, bound).astype(dtype)


def setup_inputs(seed: int = 0) -> dict:
    arg_keys = jax.random.split(jax.random.key(seed), 4)
    return {
        "omega": centred(arg_keys[0], (SKETCH, NROWS), (SKETCH // 16) ** -0.5, 0.5, ((0, 4), (1, 8))),
        "basis": centred(arg_keys[1], (NROWS, COLUMNS), 1.0, 6.0, ((0, 8), (1, 4))),
        "vectors": centred(arg_keys[2], (NVEC, NROWS), 1.0, 6.0, ((1, 8),)),
    }


def lower_solve(factor, right):
    return lax.linalg.triangular_solve(factor, right, left_side=True, lower=True, transpose_a=False)

def factor_solve(factor, right):
    half = lower_solve(factor, right)
    return lax.linalg.triangular_solve(factor, half, left_side=True, lower=True, transpose_a=True)

def reference(omega, basis, vectors):
    hi = lax.Precision.HIGHEST
    probe = lax.dot_general(vectors.astype(jnp.float32), omega.astype(jnp.float32), (((1,), (1,)), ((), ())), preferred_element_type=jnp.float32)
    remain = vectors.astype(jnp.float32)
    pieces = []
    for block_id in range(N_SECTION):
        columns = basis[:, block_id * BLOCK:(block_id + 1) * BLOCK]
        sketch = jnp.dot(omega.astype(jnp.float32), columns.astype(jnp.float32), preferred_element_type=jnp.float32)
        gram = jnp.dot(sketch.T, sketch, precision=hi)
        factor = jnp.linalg.cholesky(gram)
        inner = jnp.dot(probe, sketch, precision=hi)
        coef = factor_solve(factor, inner.T).T
        probe = probe - jnp.dot(coef, sketch.T, precision=hi)
        pieces.append(coef)
        rounded = coef.astype(jnp.bfloat16)
        remain = remain - lax.dot_general(rounded.astype(jnp.float32), columns.astype(jnp.float32), (((1,), (1,)), ((), ())), preferred_element_type=jnp.float32)
    small = jnp.dot(probe, probe.T, precision=hi)
    lower = jnp.linalg.cholesky(small)
    ortho = lower_solve(lower, remain)
    return (ortho, jnp.concatenate(pieces, axis=1))
```

```python
import functools

import jax
import jax.numpy as jnp
from jax import lax
from jax.experimental import pallas as pl
from jax.experimental.pallas import tpu as pltpu
from jax.sharding import PartitionSpec as P

MESH = pl.DeviceIdType.MESH
HI = lax.Precision.HIGHEST
F32 = jnp.float32
BF16 = jnp.bfloat16
PAD = 8


def remote(src, dst, send, recv, axis, index):
    return pltpu.make_async_remote_copy(
        src_ref=src, dst_ref=dst, send_sem=send, recv_sem=recv,
        device_id={axis: index}, device_id_type=MESH,
    )


def each(first, count, fn):
    def step(t, carry):
        fn(t)
        return carry

    lax.fori_loop(first, count, step, 0)


def greet(pairs):
    barrier = pltpu.get_barrier_semaphore()
    total = 0
    for axis, count in pairs:
        me = lax.axis_index(axis)

        def hello(t, axis=axis, count=count, me=me):
            pl.semaphore_signal(
                barrier, inc=1, device_id={axis: lax.rem(me + t, count)}, device_id_type=MESH
            )

        each(1, count, hello)
        total += count - 1
    pl.semaphore_wait(barrier, total)


def sketch_kernel(
    ns, nr, omega, basis, vec, s_out, x_out, c_out, p_out, b_out,
    bg, acc, pslot, hs, zslot, xs, xsend, cs, csend, pvs, pbuf, cg,
    bsend, brecv, psend, precv, qsend, qrecv, zsend, zrecv,
    asend, arecv, fsend, frecv, xsnd, xrcv, csnd, crcv,
    gsend, grecv, hsend, hrecv, ksend, krecv,
):
    me = lax.axis_index("section")
    row = lax.axis_index("row")
    nz = nr // 2
    z, c = row // 2, lax.rem(row, 2)
    partner = z * 2 + 1 - c
    m, width = omega.shape[0], basis.shape[1]
    half = m // 2
    ch = half // nz
    span = pbuf.shape[0]
    mine = c * nz + z
    greet((("section", ns), ("row", nr)))

    def basis_copy(t):
        peer = lax.rem(me + t, ns)
        return remote(basis, bg.at[me], bsend.at[t], brecv.at[me], "section", peer)

    each(1, ns, lambda t: basis_copy(t).start())
    bg[me] = basis[...]
    pvs[row] = lax.dot_general(
        vec[...], omega[...], (((1,), (1,)), ((), ())), preferred_element_type=F32
    )[:PAD]

    def probe_copy(t, slot):
        return remote(
            pvs.at[slot], pvs.at[slot], psend.at[t], precv.at[slot], "row", lax.rem(row + t, nr)
        )

    each(1, nr, lambda t: probe_copy(t, row).start())

    def pair_copy(j):
        other = pl.multiple_of((1 - c) * half, half)
        return remote(
            acc.at[j, pl.ds(other, half)], pslot.at[j], qsend.at[j], qrecv.at[j], "row", partner
        )

    def z_copy(j, t, slot):
        to = lax.rem(z + t, nz)
        return remote(
            hs.at[j, to], zslot.at[j, slot], zsend.at[j, t], zrecv.at[j, slot], "row", to * 2 + c
        )

    def a_copy(j, t, slot):
        to = lax.rem(z + t, nz)
        chunk = s_out.at[j, c * nz + slot]
        return remote(chunk, chunk, asend.at[j, t], arecv.at[j, slot], "row", to * 2 + c)

    def f_copy(j, core, slot):
        chunk = s_out.at[j, core * nz + slot]
        return remote(chunk, chunk, fsend.at[j, slot], frecv.at[j, slot], "row", partner)

    def c_copy(t):
        to = lax.rem(me + t, ns)
        return remote(csend.at[to], cs.at[me], csnd.at[t], crcv.at[me], "section", to)

    def block(t):
        return lax.rem(me + t, ns)

    def partial_stage(t):
        j = block(t)

        @pl.when(t > 0)
        def _():
            remote(basis, bg.at[j], bsend.at[0], brecv.at[j], "section", j).wait_recv()

        acc[j] = jnp.dot(omega[...], bg[j], preferred_element_type=F32)
        pair_copy(j).start()
        pair_copy(j).wait_recv()
        own = pl.multiple_of(c * half, half)
        total = acc[j, pl.ds(own, half)] + pslot[j]
        pslot[j] = total
        hs[j] = total.reshape(nz, ch, width)
        each(1, nz, lambda s: z_copy(j, s, z).start())

    def sum_stage(t):
        j = block(t)
        each(1, nz, lambda s: z_copy(j, s, lax.rem(z + s, nz)).wait_recv())
        total = pslot[j, pl.ds(pl.multiple_of(z * ch, ch), ch)]
        for s in range(1, nz):
            total = total + zslot[j, lax.rem(z + s, nz)]
        s_out[j, mine] = total.astype(BF16)
        each(1, nz, lambda s: a_copy(j, s, z).start())
        f_copy(j, c, z).start()
        first = mine * ch
        base = pl.multiple_of(first // span * span, span)
        inner = pl.multiple_of(lax.rem(first, span), ch)
        pbuf[...] = jnp.zeros_like(pbuf)
        pbuf[pl.ds(inner, ch), :] = total
        csend[j] = jnp.dot(
            p_out[:, pl.ds(base, span)], pbuf[...], precision=HI, preferred_element_type=F32
        )
        pl.when(t > 0)(lambda: c_copy(t).start())

    def forward_stage(t):
        j = block(t)

        def one(s):
            slot = lax.rem(z + s, nz)
            a_copy(j, s, slot).wait_recv()
            f_copy(j, c, slot).start()

        each(1, nz, one)

    def loop(t):
        pl.when(t < ns)(lambda: partial_stage(t))
        pl.when((t >= 1) & (t < ns + 1))(lambda: sum_stage(t - 1))
        pl.when(t >= 2)(lambda: forward_stage(t - 2))

    partial_stage(0)
    each(1, nr, lambda t: probe_copy(t, lax.rem(row + t, nr)).wait_recv())
    probe = pvs[0]
    for k in range(1, nr):
        probe = probe + pvs[k]
    p_out[...] = probe
    each(1, ns + 2, loop)
    each(0, ns, lambda j: each(0, nz, lambda s: f_copy(j, 1 - c, s).wait_recv()))

    w = ns * width // nr
    left = row * w // width
    if w < width:
        off = pl.multiple_of(lax.rem(row * w, width), w)
        part = s_out[left, :, :, pl.ds(off, w)]
    else:
        part = s_out[left]
    part = part.reshape(m, w).astype(F32).T.astype(BF16)

    def x_copy(t):
        to = lax.rem(me + t, ns)
        return remote(xsend.at[to], xs.at[me], xsnd.at[t], xrcv.at[me], "section", to)

    def gram_of(i):
        right = s_out[i].reshape(m, width)
        xsend[i] = jnp.dot(part, right, preferred_element_type=F32)

    def gram_stage(t):
        gram_of(lax.rem(me + t, ns))
        x_copy(t).start()

    each(1, ns, gram_stage)
    gram_of(me)

    def gather(t):
        i = lax.rem(me + t, ns)
        remote(xsend.at[i], xs.at[i], xsnd.at[0], xrcv.at[i], "section", i).wait_recv()
        remote(csend.at[i], cs.at[i], csnd.at[0], crcv.at[i], "section", i).wait_recv()

    each(1, ns, gather)
    xt, ct = xsend[me], csend[me]
    for t in range(1, ns):
        i = lax.rem(me + t, ns)
        xt = xt + xs[i]
        ct = ct + cs[i]
    cg[row] = ct
    x_out[row] = xt

    def k_copy(t, slot):
        return remote(
            cg.at[slot], cg.at[slot], ksend.at[t], krecv.at[slot], "row", lax.rem(row + t, nr)
        )

    each(1, nr, lambda t: k_copy(t, row).start())

    def g_copy(t, slot):
        to = lax.rem(z + t, nz)
        piece = x_out.at[slot * 2 + c]
        return remote(piece, piece, gsend.at[t], grecv.at[slot], "row", to * 2 + c)

    def h_copy(core, slot):
        piece = x_out.at[slot * 2 + core]
        return remote(piece, piece, hsend.at[slot], hrecv.at[slot], "row", partner)

    each(1, nz, lambda s: g_copy(s, z).start())
    h_copy(c, z).start()

    rows = b_out.shape[1]
    start = pl.multiple_of(me * rows, rows)
    b_out[...] = bg[:, pl.ds(start, rows), :]

    def pass_on(s):
        slot = lax.rem(z + s, nz)
        g_copy(s, slot).wait_recv()
        h_copy(c, slot).start()

    each(1, nz, pass_on)
    each(0, nz, lambda s: h_copy(1 - c, s).wait_recv())
    each(1, nr, lambda t: k_copy(t, lax.rem(row + t, nr)).wait_recv())
    ct = cg[0]
    for k in range(1, nr):
        ct = ct + cg[k]
    c_out[...] = ct

    each(1, nr, lambda t: k_copy(t, row).wait_send())
    each(1, ns, lambda t: basis_copy(t).wait_send())
    each(1, nr, lambda t: probe_copy(t, row).wait_send())

    def drain(j):
        pair_copy(j).wait_send()
        each(1, nz, lambda s: z_copy(j, s, z).wait_send())
        each(1, nz, lambda s: a_copy(j, s, z).wait_send())
        each(0, nz, lambda s: f_copy(j, c, s).wait_send())

    each(0, ns, drain)
    each(1, ns, lambda t: x_copy(t).wait_send())
    each(1, ns, lambda t: c_copy(t).wait_send())
    each(1, nz, lambda s: g_copy(s, z).wait_send())
    each(0, nz, lambda s: h_copy(c, s).wait_send())


def solve_kernel(
    ns, n, x, inv, c0, s_in, p0, b, vec, ortho, coef,
    rbuf, cur, sm, rsend, rrecv, ssend, srecv,
):
    me = lax.axis_index("section")
    m, width = p0.shape[1], c0.shape[1]
    greet((("section", ns),))
    cur[...] = c0[...]

    def r_copy(t, slot):
        return remote(
            rbuf.at[slot], rbuf.at[slot], rsend.at[t], rrecv.at[slot],
            "section", lax.rem(me + t, ns),
        )

    def chain(j):
        @pl.when(me == j)
        def _():
            mid = lax.dot_general(
                cur[...], inv[...], (((1,), (1,)), ((), ())), precision=HI,
                preferred_element_type=F32,
            )
            rbuf[me] = jnp.dot(mid, inv[...], precision=HI, preferred_element_type=F32)
            each(1, ns, lambda t: r_copy(t, me).start())

        @pl.when(me != j)
        def _():
            remote(rbuf.at[j], rbuf.at[j], rsend.at[0], rrecv.at[j], "section", j).wait_recv()

        @pl.when(me > j)
        def _():
            cur[...] -= jnp.dot(rbuf[j], x[j], precision=HI, preferred_element_type=F32)

    each(0, ns, chain)

    def fold(j, carry):
        probe, remain = carry
        r = rbuf[j]
        sj = s_in[j].reshape(m, width).astype(F32)
        nt = (((1,), (1,)), ((), ()))
        probe = probe - lax.dot_general(r, sj, nt, precision=HI, preferred_element_type=F32)
        rb = jnp.concatenate([r, r], axis=0).astype(BF16)
        remain = remain - lax.dot_general(rb, b[j], nt, preferred_element_type=F32)[:PAD]
        return probe, remain

    probe, remain = lax.fori_loop(0, ns, fold, (p0[...], vec[...]))
    small = lax.dot_general(
        probe, probe, (((1,), (1,)), ((), ())), precision=HI, preferred_element_type=F32
    )
    sm[me] = jnp.concatenate([small, jnp.zeros((PAD, 128 - PAD), F32)], axis=1)

    def s_copy(t, slot):
        return remote(
            sm.at[slot], sm.at[slot], ssend.at[t], srecv.at[slot],
            "section", lax.rem(me + t, ns),
        )

    each(1, ns, lambda t: s_copy(t, me).start())
    coef[...] = rbuf[me, :n]
    each(1, ns, lambda t: s_copy(t, lax.rem(me + t, ns)).wait_recv())
    full = sm[0]
    for k in range(1, ns):
        full = full + sm[k]
    low = {}
    rows = []
    for i in range(n):
        for k in range(i + 1):
            value = full[i:i + 1, k:k + 1]
            for q in range(k):
                value = value - low[i, q] * low[k, q]
            low[i, k] = jnp.sqrt(value) if i == k else value / low[k, k]
        line = remain[i:i + 1]
        for k in range(i):
            line = line - low[i, k] * rows[k]
        rows.append(line / low[i, i])
        ortho[i:i + 1, :] = rows[i]
    each(1, ns, lambda t: r_copy(t, me).wait_send())
    each(1, ns, lambda t: s_copy(t, me).wait_send())


def body(ns, nr, omega, basis, vectors):
    dma = pltpu.SemaphoreType.DMA
    n, k = vectors.shape
    m, width = omega.shape[0], basis.shape[1]
    nz = nr // 2
    half = m // 2
    ch = half // nz
    w = ns * width // nr
    rows = k // ns
    vmem = pl.BlockSpec(memory_space=pltpu.VMEM)
    padded = jnp.pad(vectors, ((0, 2 * PAD - n), (0, 0)))
    s_all, x, c0, p0, b = pl.pallas_call(
        functools.partial(sketch_kernel, ns, nr),
        out_shape=(
            jax.ShapeDtypeStruct((ns, nr, ch, width), BF16),
            jax.ShapeDtypeStruct((nr, w, width), F32),
            jax.ShapeDtypeStruct((PAD, width), F32),
            jax.ShapeDtypeStruct((PAD, m), F32),
            jax.ShapeDtypeStruct((ns, rows, width), BF16),
        ),
        in_specs=[vmem] * 3,
        out_specs=(vmem,) * 5,
        scratch_shapes=[
            pltpu.VMEM((ns, k, width), BF16),
            pltpu.VMEM((ns, m, width), F32),
            pltpu.VMEM((ns, half, width), F32),
            pltpu.VMEM((ns, nz, ch, width), F32),
            pltpu.VMEM((ns, nz, ch, width), F32),
            pltpu.VMEM((ns, w, width), F32),
            pltpu.VMEM((ns, w, width), F32),
            pltpu.VMEM((ns, PAD, width), F32),
            pltpu.VMEM((ns, PAD, width), F32),
            pltpu.VMEM((nr, PAD, m), F32),
            pltpu.VMEM((max(ch, 128), width), F32),
            pltpu.VMEM((nr, PAD, width), F32),
            dma((ns,)), dma((ns,)), dma((nr,)), dma((nr,)), dma((ns,)), dma((ns,)),
            dma((ns, nz)), dma((ns, nz)), dma((ns, nz)), dma((ns, nz)),
            dma((ns, nz)), dma((ns, nz)), dma((ns,)), dma((ns,)), dma((ns,)), dma((ns,)),
            dma((nz,)), dma((nz,)), dma((nz,)), dma((nz,)), dma((nr,)), dma((nr,)),
        ],
        compiler_params=pltpu.CompilerParams(
            collective_id=0, has_side_effects=True, vmem_limit_bytes=60 * 2**20
        ),
    )(omega, basis, padded)
    x = x.reshape(ns, width, width)
    me = lax.axis_index("section")
    gram = lax.dynamic_index_in_dim(x, me, 0, keepdims=False)
    factor = jnp.linalg.cholesky(gram, symmetrize_input=False)
    inv = lax.linalg.triangular_solve(
        factor, jnp.eye(width, dtype=F32), left_side=True, lower=True, transpose_a=False
    )
    mine = lax.dynamic_slice_in_dim(vectors, me * rows, rows, 1).astype(F32)
    mine = jnp.pad(mine, ((0, PAD - n), (0, 0)))
    return pl.pallas_call(
        functools.partial(solve_kernel, ns, n),
        out_shape=(
            jax.ShapeDtypeStruct((n, rows), F32),
            jax.ShapeDtypeStruct((n, width), F32),
        ),
        in_specs=[vmem] * 7,
        out_specs=(vmem,) * 2,
        scratch_shapes=[
            pltpu.VMEM((ns, PAD, width), F32),
            pltpu.VMEM((PAD, width), F32),
            pltpu.VMEM((ns, PAD, 128), F32),
            dma((ns,)), dma((ns,)), dma((ns,)), dma((ns,)),
        ],
        compiler_params=pltpu.CompilerParams(
            collective_id=1, has_side_effects=True, vmem_limit_bytes=60 * 2**20
        ),
    )(x, inv, c0, s_all, p0, b, mine)


def solution(mesh):
    return jax.shard_map(
        functools.partial(body, mesh.shape["section"], mesh.shape["row"]),
        mesh=mesh,
        in_specs=(P("section", "row"), P("row", "section"), P(None, "row")),
        out_specs=(P(None, ("row", "section")), P(None, "section")),
        check_vma=False,
    )
```

```python
import functools

import jax
import jax.numpy as jnp
from jax import lax
from jax.experimental import pallas as pl
from jax.experimental.pallas import tpu as pltpu
from jax.sharding import PartitionSpec as P

MESH = pl.DeviceIdType.MESH
HI = lax.Precision.HIGHEST
F32 = jnp.float32
BF16 = jnp.bfloat16
PAD = 8


def remote(src, dst, send, recv, axis, index):
    return pltpu.make_async_remote_copy(
        src_ref=src, dst_ref=dst, send_sem=send, recv_sem=recv,
        device_id={axis: index}, device_id_type=MESH,
    )


def each(first, count, fn):
    def step(t, carry):
        fn(t)
        return carry

    lax.fori_loop(first, count, step, 0)


def greet(pairs):
    barrier = pltpu.get_barrier_semaphore()
    total = 0
    for axis, count in pairs:
        me = lax.axis_index(axis)

        def hello(t, axis=axis, count=count, me=me):
            pl.semaphore_signal(
                barrier, inc=1, device_id={axis: lax.rem(me + t, count)}, device_id_type=MESH
            )

        each(1, count, hello)
        total += count - 1
    pl.semaphore_wait(barrier, total)


def sketch_kernel(
    ns, nr, omega, basis, vec, s_out, x_out, c_out, p_out, b_out,
    bg, acc, pslot, hs, zslot, xs, xsend, cs, csend, pvs, pbuf, cg,
    bsend, brecv, psend, precv, qsend, qrecv, zsend, zrecv,
    asend, arecv, fsend, frecv, xsnd, xrcv, csnd, crcv,
    gsend, grecv, hsend, hrecv, ksend, krecv,
):
    me = lax.axis_index("section")
    row = lax.axis_index("row")
    nz = nr // 2
    z, c = row // 2, lax.rem(row, 2)
    partner = z * 2 + 1 - c
    m, width = omega.shape[0], basis.shape[1]
    half = m // 2
    ch = half // nz
    span = pbuf.shape[0]
    mine = c * nz + z
    greet((("section", ns), ("row", nr)))

    def basis_copy(t):
        peer = lax.rem(me + t, ns)
        return remote(basis, bg.at[me], bsend.at[t], brecv.at[me], "section", peer)

    each(1, ns, lambda t: basis_copy(t).start())
    bg[me] = basis[...]
    pvs[row] = lax.dot_general(
        vec[...], omega[...], (((1,), (1,)), ((), ())), preferred_element_type=F32
    )[:PAD]

    def probe_copy(t, slot):
        return remote(
            pvs.at[slot], pvs.at[slot], psend.at[t], precv.at[slot], "row", lax.rem(row + t, nr)
        )

    each(1, nr, lambda t: probe_copy(t, row).start())

    def pair_copy(j):
        other = pl.multiple_of((1 - c) * half, half)
        return remote(
            acc.at[j, pl.ds(other, half)], pslot.at[j], qsend.at[j], qrecv.at[j], "row", partner
        )

    def z_copy(j, t, slot):
        to = lax.rem(z + t, nz)
        return remote(
            hs.at[j, to], zslot.at[j, slot], zsend.at[j, t], zrecv.at[j, slot], "row", to * 2 + c
        )

    def a_copy(j, t, slot):
        to = lax.rem(z + t, nz)
        chunk = s_out.at[j, c * nz + slot]
        return remote(chunk, chunk, asend.at[j, t], arecv.at[j, slot], "row", to * 2 + c)

    def f_copy(j, core, slot):
        chunk = s_out.at[j, core * nz + slot]
        return remote(chunk, chunk, fsend.at[j, slot], frecv.at[j, slot], "row", partner)

    def c_copy(t):
        to = lax.rem(me + t, ns)
        return remote(csend.at[to], cs.at[me], csnd.at[t], crcv.at[me], "section", to)

    def block(t):
        return lax.rem(me + t, ns)

    def partial_stage(t):
        j = block(t)

        @pl.when(t > 0)
        def _():
            remote(basis, bg.at[j], bsend.at[0], brecv.at[j], "section", j).wait_recv()

        acc[j] = jnp.dot(omega[...], bg[j], preferred_element_type=F32)
        pair_copy(j).start()
        pair_copy(j).wait_recv()
        own = pl.multiple_of(c * half, half)
        total = acc[j, pl.ds(own, half)] + pslot[j]
        pslot[j] = total
        hs[j] = total.reshape(nz, ch, width)
        each(1, nz, lambda s: z_copy(j, s, z).start())

    def sum_stage(t):
        j = block(t)
        each(1, nz, lambda s: z_copy(j, s, lax.rem(z + s, nz)).wait_recv())
        total = pslot[j, pl.ds(pl.multiple_of(z * ch, ch), ch)]
        for s in range(1, nz):
            total = total + zslot[j, lax.rem(z + s, nz)]
        s_out[j, mine] = total.astype(BF16)
        each(1, nz, lambda s: a_copy(j, s, z).start())
        f_copy(j, c, z).start()
        first = mine * ch
        base = pl.multiple_of(first // span * span, span)
        inner = pl.multiple_of(lax.rem(first, span), ch)
        pbuf[...] = jnp.zeros_like(pbuf)
        pbuf[pl.ds(inner, ch), :] = total
        csend[j] = jnp.dot(
            p_out[:, pl.ds(base, span)], pbuf[...], precision=HI, preferred_element_type=F32
        )
        pl.when(t > 0)(lambda: c_copy(t).start())

    def forward_stage(t):
        j = block(t)

        def one(s):
            slot = lax.rem(z + s, nz)
            a_copy(j, s, slot).wait_recv()
            f_copy(j, c, slot).start()

        each(1, nz, one)

    def loop(t):
        pl.when(t < ns)(lambda: partial_stage(t))
        pl.when((t >= 1) & (t < ns + 1))(lambda: sum_stage(t - 1))
        pl.when(t >= 2)(lambda: forward_stage(t - 2))

    partial_stage(0)
    each(1, nr, lambda t: probe_copy(t, lax.rem(row + t, nr)).wait_recv())
    probe = pvs[0]
    for k in range(1, nr):
        probe = probe + pvs[k]
    p_out[...] = probe
    each(1, ns + 2, loop)
    each(0, ns, lambda j: each(0, nz, lambda s: f_copy(j, 1 - c, s).wait_recv()))

    w = ns * width // nr
    left = row * w // width
    if w < width:
        off = pl.multiple_of(lax.rem(row * w, width), w)
        part = s_out[left, :, :, pl.ds(off, w)]
    else:
        part = s_out[left]
    part = part.reshape(m, w).astype(F32).T.astype(BF16)

    def x_copy(t):
        to = lax.rem(me + t, ns)
        return remote(xsend.at[to], xs.at[me], xsnd.at[t], xrcv.at[me], "section", to)

    def gram_of(i):
        right = s_out[i].reshape(m, width)
        xsend[i] = jnp.dot(part, right, preferred_element_type=F32)

    def gram_stage(t):
        gram_of(lax.rem(me + t, ns))
        x_copy(t).start()

    each(1, ns, gram_stage)
    gram_of(me)

    def gather(t):
        i = lax.rem(me + t, ns)
        remote(xsend.at[i], xs.at[i], xsnd.at[0], xrcv.at[i], "section", i).wait_recv()
        remote(csend.at[i], cs.at[i], csnd.at[0], crcv.at[i], "section", i).wait_recv()

    each(1, ns, gather)
    xt, ct = xsend[me], csend[me]
    for t in range(1, ns):
        i = lax.rem(me + t, ns)
        xt = xt + xs[i]
        ct = ct + cs[i]
    cg[row] = ct
    x_out[row] = xt

    def k_copy(t, slot):
        return remote(
            cg.at[slot], cg.at[slot], ksend.at[t], krecv.at[slot], "row", lax.rem(row + t, nr)
        )

    each(1, nr, lambda t: k_copy(t, row).start())

    def g_copy(t, slot):
        to = lax.rem(z + t, nz)
        piece = x_out.at[slot * 2 + c]
        return remote(piece, piece, gsend.at[t], grecv.at[slot], "row", to * 2 + c)

    def h_copy(core, slot):
        piece = x_out.at[slot * 2 + core]
        return remote(piece, piece, hsend.at[slot], hrecv.at[slot], "row", partner)

    each(1, nz, lambda s: g_copy(s, z).start())
    h_copy(c, z).start()

    rows = b_out.shape[1]
    start = pl.multiple_of(me * rows, rows)
    b_out[...] = bg[:, pl.ds(start, rows), :]

    def pass_on(s):
        slot = lax.rem(z + s, nz)
        g_copy(s, slot).wait_recv()
        h_copy(c, slot).start()

    each(1, nz, pass_on)
    each(0, nz, lambda s: h_copy(1 - c, s).wait_recv())
    each(1, nr, lambda t: k_copy(t, lax.rem(row + t, nr)).wait_recv())
    ct = cg[0]
    for k in range(1, nr):
        ct = ct + cg[k]
    c_out[...] = ct

    each(1, nr, lambda t: k_copy(t, row).wait_send())
    each(1, ns, lambda t: basis_copy(t).wait_send())
    each(1, nr, lambda t: probe_copy(t, row).wait_send())

    def drain(j):
        pair_copy(j).wait_send()
        each(1, nz, lambda s: z_copy(j, s, z).wait_send())
        each(1, nz, lambda s: a_copy(j, s, z).wait_send())
        each(0, nz, lambda s: f_copy(j, c, s).wait_send())

    each(0, ns, drain)
    each(1, ns, lambda t: x_copy(t).wait_send())
    each(1, ns, lambda t: c_copy(t).wait_send())
    each(1, nz, lambda s: g_copy(s, z).wait_send())
    each(0, nz, lambda s: h_copy(c, s).wait_send())


def invert_tile(mat):
    size = mat.shape[0]
    lane = lax.broadcasted_iota(jnp.int32, (size, size), 1)
    sub = lax.broadcasted_iota(jnp.int32, (PAD, size), 0)
    short = lax.broadcasted_iota(jnp.int32, (PAD, size), 1)
    for k in range(0, size, PAD):
        cols = [jnp.broadcast_to(mat[:, k + q:k + q + 1], (size, size)) for q in range(PAD)]
        heads = [col[k:k + PAD] for col in cols]
        rows = jnp.where((short >= k) & (short < k + PAD), 0.0, mat[k:k + PAD])
        rows = rows + jnp.where(short == sub + k, 1.0, 0.0)
        for p in range(PAD):
            scale = 1.0 / heads[p][p:p + 1]
            line = rows[p:p + 1] * scale
            rows = jnp.where(sub == p, line, rows - heads[p] * line)
            for q in range(p + 1, PAD):
                head = heads[q][p:p + 1] * scale
                heads[q] = jnp.where(sub == p, head, heads[q] - heads[p] * head)
        mat = jnp.where((lane >= k) & (lane < k + PAD), 0.0, mat)
        for q in range(PAD):
            mat = mat - cols[q] * rows[q:q + 1]
        parts = [mat[:k], rows, mat[k + PAD:]]
        mat = jnp.concatenate([part for part in parts if part.shape[0]], axis=0)
    return mat


def invert_kernel(x, inv):
    width = inv.shape[0]
    size = min(width, 128)
    inv[...] = x[lax.axis_index("section")]
    column = lax.broadcasted_iota(jnp.int32, (width, width), 1) // size
    eye = (
        lax.broadcasted_iota(jnp.int32, (size, size), 0)
        == lax.broadcasted_iota(jnp.int32, (size, size), 1)
    ).astype(F32)

    def step(b, carry):
        at = pl.ds(pl.multiple_of(b * size, size), size)
        pivot = invert_tile(inv[at, at])
        left = inv[:, at]
        inv[at, at] = eye
        rows = jnp.dot(pivot, inv[at, :], precision=HI, preferred_element_type=F32)
        rest = jnp.where(column == b, 0.0, inv[...])
        inv[...] = rest - jnp.dot(left, rows, precision=HI, preferred_element_type=F32)
        inv[at, :] = rows
        return carry

    lax.fori_loop(0, width // size, step, 0)


def solve_kernel(
    ns, n, x, inv, c0, s_in, p0, b, vec, ortho, coef,
    rbuf, cur, sm, rsend, rrecv, ssend, srecv,
):
    me = lax.axis_index("section")
    m, width = p0.shape[1], c0.shape[1]
    greet((("section", ns),))
    cur[...] = c0[...]

    def r_copy(t, slot):
        return remote(
            rbuf.at[slot], rbuf.at[slot], rsend.at[t], rrecv.at[slot],
            "section", lax.rem(me + t, ns),
        )

    def chain(j):
        @pl.when(me == j)
        def _():
            rbuf[me] = jnp.dot(cur[...], inv[...], precision=HI, preferred_element_type=F32)
            each(1, ns, lambda t: r_copy(t, me).start())

        @pl.when(me != j)
        def _():
            remote(rbuf.at[j], rbuf.at[j], rsend.at[0], rrecv.at[j], "section", j).wait_recv()

        @pl.when(me > j)
        def _():
            cur[...] -= jnp.dot(rbuf[j], x[j], precision=HI, preferred_element_type=F32)

    each(0, ns, chain)

    def fold(j, carry):
        probe, remain = carry
        r = rbuf[j]
        sj = s_in[j].reshape(m, width).astype(F32)
        nt = (((1,), (1,)), ((), ()))
        probe = probe - lax.dot_general(r, sj, nt, precision=HI, preferred_element_type=F32)
        rb = jnp.concatenate([r, r], axis=0).astype(BF16)
        remain = remain - lax.dot_general(rb, b[j], nt, preferred_element_type=F32)[:PAD]
        return probe, remain

    probe, remain = lax.fori_loop(0, ns, fold, (p0[...], vec[...]))
    small = lax.dot_general(
        probe, probe, (((1,), (1,)), ((), ())), precision=HI, preferred_element_type=F32
    )
    sm[me] = jnp.concatenate([small, jnp.zeros((PAD, 128 - PAD), F32)], axis=1)

    def s_copy(t, slot):
        return remote(
            sm.at[slot], sm.at[slot], ssend.at[t], srecv.at[slot],
            "section", lax.rem(me + t, ns),
        )

    each(1, ns, lambda t: s_copy(t, me).start())
    coef[...] = rbuf[me, :n]
    each(1, ns, lambda t: s_copy(t, lax.rem(me + t, ns)).wait_recv())
    full = sm[0]
    for k in range(1, ns):
        full = full + sm[k]
    low = {}
    rows = []
    for i in range(n):
        for k in range(i + 1):
            value = full[i:i + 1, k:k + 1]
            for q in range(k):
                value = value - low[i, q] * low[k, q]
            low[i, k] = jnp.sqrt(value) if i == k else value / low[k, k]
        line = remain[i:i + 1]
        for k in range(i):
            line = line - low[i, k] * rows[k]
        rows.append(line / low[i, i])
        ortho[i:i + 1, :] = rows[i]
    each(1, ns, lambda t: r_copy(t, me).wait_send())
    each(1, ns, lambda t: s_copy(t, me).wait_send())


def body(ns, nr, omega, basis, vectors):
    dma = pltpu.SemaphoreType.DMA
    n, k = vectors.shape
    m, width = omega.shape[0], basis.shape[1]
    nz = nr // 2
    half = m // 2
    ch = half // nz
    w = ns * width // nr
    rows = k // ns
    vmem = pl.BlockSpec(memory_space=pltpu.VMEM)
    padded = jnp.pad(vectors, ((0, 2 * PAD - n), (0, 0)))
    s_all, x, c0, p0, b = pl.pallas_call(
        functools.partial(sketch_kernel, ns, nr),
        out_shape=(
            jax.ShapeDtypeStruct((ns, nr, ch, width), BF16),
            jax.ShapeDtypeStruct((nr, w, width), F32),
            jax.ShapeDtypeStruct((PAD, width), F32),
            jax.ShapeDtypeStruct((PAD, m), F32),
            jax.ShapeDtypeStruct((ns, rows, width), BF16),
        ),
        in_specs=[vmem] * 3,
        out_specs=(vmem,) * 5,
        scratch_shapes=[
            pltpu.VMEM((ns, k, width), BF16),
            pltpu.VMEM((ns, m, width), F32),
            pltpu.VMEM((ns, half, width), F32),
            pltpu.VMEM((ns, nz, ch, width), F32),
            pltpu.VMEM((ns, nz, ch, width), F32),
            pltpu.VMEM((ns, w, width), F32),
            pltpu.VMEM((ns, w, width), F32),
            pltpu.VMEM((ns, PAD, width), F32),
            pltpu.VMEM((ns, PAD, width), F32),
            pltpu.VMEM((nr, PAD, m), F32),
            pltpu.VMEM((max(ch, 128), width), F32),
            pltpu.VMEM((nr, PAD, width), F32),
            dma((ns,)), dma((ns,)), dma((nr,)), dma((nr,)), dma((ns,)), dma((ns,)),
            dma((ns, nz)), dma((ns, nz)), dma((ns, nz)), dma((ns, nz)),
            dma((ns, nz)), dma((ns, nz)), dma((ns,)), dma((ns,)), dma((ns,)), dma((ns,)),
            dma((nz,)), dma((nz,)), dma((nz,)), dma((nz,)), dma((nr,)), dma((nr,)),
        ],
        compiler_params=pltpu.CompilerParams(
            collective_id=0, has_side_effects=True, vmem_limit_bytes=60 * 2**20
        ),
    )(omega, basis, padded)
    x = x.reshape(ns, width, width)
    me = lax.axis_index("section")
    inv = pl.pallas_call(
        invert_kernel,
        out_shape=jax.ShapeDtypeStruct((width, width), F32),
        in_specs=[vmem],
        out_specs=vmem,
        compiler_params=pltpu.CompilerParams(vmem_limit_bytes=32 * 2**20),
    )(x)
    mine = lax.dynamic_slice_in_dim(vectors, me * rows, rows, 1).astype(F32)
    mine = jnp.pad(mine, ((0, PAD - n), (0, 0)))
    return pl.pallas_call(
        functools.partial(solve_kernel, ns, n),
        out_shape=(
            jax.ShapeDtypeStruct((n, rows), F32),
            jax.ShapeDtypeStruct((n, width), F32),
        ),
        in_specs=[vmem] * 7,
        out_specs=(vmem,) * 2,
        scratch_shapes=[
            pltpu.VMEM((ns, PAD, width), F32),
            pltpu.VMEM((PAD, width), F32),
            pltpu.VMEM((ns, PAD, 128), F32),
            dma((ns,)), dma((ns,)), dma((ns,)), dma((ns,)),
        ],
        compiler_params=pltpu.CompilerParams(
            collective_id=1, has_side_effects=True, vmem_limit_bytes=60 * 2**20
        ),
    )(x, inv, c0, s_all, p0, b, mine)


def solution(mesh):
    return jax.shard_map(
        functools.partial(body, mesh.shape["section"], mesh.shape["row"]),
        mesh=mesh,
        in_specs=(P("section", "row"), P("row", "section"), P(None, "row")),
        out_specs=(P(None, ("row", "section")), P(None, "section")),
        check_vma=False,
    )
```

```python
import functools

import jax
import jax.numpy as jnp
from jax import lax
from jax.experimental import pallas as pl
from jax.experimental.pallas import tpu as pltpu
from jax.sharding import PartitionSpec as P

MESH = pl.DeviceIdType.MESH
HI = lax.Precision.HIGHEST
F32 = jnp.float32
BF16 = jnp.bfloat16
PAD = 8


def remote(src, dst, send, recv, axis, index):
    return pltpu.make_async_remote_copy(
        src_ref=src, dst_ref=dst, send_sem=send, recv_sem=recv,
        device_id={axis: index}, device_id_type=MESH,
    )


def each(first, count, fn):
    def step(t, carry):
        fn(t)
        return carry

    lax.fori_loop(first, count, step, 0)


def greet(pairs):
    barrier = pltpu.get_barrier_semaphore()
    total = 0
    for axis, count in pairs:
        me = lax.axis_index(axis)

        def hello(t, axis=axis, count=count, me=me):
            pl.semaphore_signal(
                barrier, inc=1, device_id={axis: lax.rem(me + t, count)}, device_id_type=MESH
            )

        each(1, count, hello)
        total += count - 1
    pl.semaphore_wait(barrier, total)


class Line:
    def __init__(self, z, nz, c, chunk, up, down, recv, fsend, frecv):
        self.z, self.nz, self.c, self.chunk = z, nz, c, chunk
        self.up, self.down, self.recv = up, down, recv
        self.fsend, self.frecv = fsend, frecv

    def rise(self, slot):
        piece = self.chunk(self.c, slot)
        to = (self.z + 1) * 2 + self.c
        return remote(piece, piece, self.up(slot), self.recv(slot), "row", to)

    def sink(self, slot):
        piece = self.chunk(self.c, slot)
        to = (self.z - 1) * 2 + self.c
        return remote(piece, piece, self.down(slot), self.recv(slot), "row", to)

    def across(self, core, slot):
        piece = self.chunk(core, slot)
        to = self.z * 2 + 1 - self.c
        return remote(piece, piece, self.fsend(slot), self.frecv(slot), "row", to)

    def send(self, slot, upward, downward):
        if upward:
            pl.when(self.z < self.nz - 1)(lambda: self.rise(slot).start())
        if downward:
            pl.when(self.z > 0)(lambda: self.sink(slot).start())
        self.across(self.c, slot).start()

    def begin(self):
        self.send(self.z, True, True)

    def relay(self, s):
        @pl.when(self.z >= s)
        def _():
            self.sink(self.z - s).wait_recv()
            self.send(self.z - s, True, False)

        @pl.when(self.z + s < self.nz)
        def _():
            self.sink(self.z + s).wait_recv()
            self.send(self.z + s, False, True)

    def finish(self):
        each(0, self.nz, lambda q: self.across(1 - self.c, q).wait_recv())

    def drain(self):
        def one(q):
            pl.when((q <= self.z) & (self.z < self.nz - 1))(lambda: self.rise(q).wait_send())
            pl.when((q >= self.z) & (self.z > 0))(lambda: self.sink(q).wait_send())
            self.across(self.c, q).wait_send()

        each(0, self.nz, one)


def sketch_kernel(
    ns, nr, omega, basis, vec, s_out, x_out, c_out, p_out, b_out,
    bg, acc, pslot, hs, zslot, xs, xsend, cs, csend, pvs, pbuf, cg,
    rsend, rrecv, lsend, lrecv, psend, precv, qsend, qrecv, zsend, zrecv,
    aup, adown, arecv, fsend, frecv, xsnd, xrcv, csnd, crcv,
    gup, gdown, grecv, hsend, hrecv, ksend, krecv, lbsem,
):
    me = lax.axis_index("section")
    row = lax.axis_index("row")
    nz = nr // 2
    z, c = row // 2, lax.rem(row, 2)
    partner = z * 2 + 1 - c
    m, width = omega.shape[0], basis.shape[1]
    half = m // 2
    ch = half // nz
    span = pbuf.shape[0]
    mine = c * nz + z
    greet((("section", ns), ("row", nr)))

    far = ns // 2
    tall = basis.shape[0] // 2

    def at_place(p):
        return jnp.where(p < far, p, ns + far - 1 - p)

    place = at_place(me)

    def near(d):
        return at_place(lax.rem(place + d + ns, ns))

    def right_copy(d, part):
        origin = near(-d)
        block = bg.at[origin, pl.ds(0, tall)] if part else bg.at[origin]
        return remote(block, block, rsend.at[d], rrecv.at[origin], "section", near(1))

    def left_copy(d, part):
        origin = near(d)
        block = bg.at[origin, pl.ds(tall, tall)] if part else bg.at[origin]
        return remote(block, block, lsend.at[d], lrecv.at[origin], "section", near(-1))

    def first_copy(send, recv, to):
        return remote(basis, bg.at[me], send.at[0], recv.at[me], "section", to)

    first_copy(rsend, rrecv, near(1)).start()
    first_copy(lsend, lrecv, near(-1)).start()
    own_block = pltpu.make_async_copy(basis, bg.at[me], lbsem)
    own_block.start()
    pvs[row] = lax.dot_general(
        vec[...], omega[...], (((1,), (1,)), ((), ())), preferred_element_type=F32
    )[:PAD]

    def probe_copy(t, slot):
        return remote(
            pvs.at[slot], pvs.at[slot], psend.at[t], precv.at[slot], "row", lax.rem(row + t, nr)
        )

    each(1, nr, lambda t: probe_copy(t, row).start())

    def pair_copy(j):
        other = pl.multiple_of((1 - c) * half, half)
        return remote(
            acc.at[j, pl.ds(other, half)], pslot.at[j], qsend.at[j], qrecv.at[j], "row", partner
        )

    def z_copy(j, t, slot):
        to = lax.rem(z + t, nz)
        return remote(
            hs.at[j, to], zslot.at[j, slot], zsend.at[j, t], zrecv.at[j, slot], "row", to * 2 + c
        )

    def line(j):
        return Line(
            z, nz, c, lambda core, slot: s_out.at[j, core * nz + slot],
            lambda q: aup.at[j, q], lambda q: adown.at[j, q], lambda q: arecv.at[j, q],
            lambda q: fsend.at[j, q], lambda q: frecv.at[j, q],
        )

    def c_copy(j):
        return remote(csend.at[j], cs.at[me], csnd.at[j], crcv.at[me], "section", j)

    def block(t):
        d = (t + 1) // 2
        return near(jnp.where(lax.rem(t, 2) == 1, ns - d, d))

    def arrive(d):
        @pl.when(d < far)
        def _():
            right_copy(d, False).wait_recv()
            left_copy(d, False).wait_recv()

            @pl.when(d + 1 < far)
            def _():
                right_copy(d, False).start()
                left_copy(d, False).start()

            @pl.when(d + 1 == far)
            def _():
                right_copy(d, True).start()
                left_copy(d, True).start()

        @pl.when(d == far)
        def _():
            right_copy(far, True).wait_recv()
            left_copy(far, True).wait_recv()

    def partial_stage(t):
        j = block(t)
        pl.when(lax.rem(t, 2) == 1)(lambda: arrive((t + 1) // 2))
        acc[j] = jnp.dot(omega[...], bg[j], preferred_element_type=F32)
        pair_copy(j).start()

    def pair_stage(t):
        j = block(t)
        pair_copy(j).wait_recv()
        own = pl.multiple_of(c * half, half)
        total = acc[j, pl.ds(own, half)] + pslot[j]
        pslot[j] = total
        hs[j] = total.reshape(nz, ch, width)
        each(1, nz, lambda s: z_copy(j, s, z).start())

    def sum_stage(t):
        j = block(t)
        each(1, nz, lambda s: z_copy(j, s, lax.rem(z + s, nz)).wait_recv())
        total = pslot[j, pl.ds(pl.multiple_of(z * ch, ch), ch)]
        for s in range(1, nz):
            total = total + zslot[j, lax.rem(z + s, nz)]
        s_out[j, mine] = total.astype(BF16)
        line(j).begin()
        first = mine * ch
        base = pl.multiple_of(first // span * span, span)
        inner = pl.multiple_of(lax.rem(first, span), ch)
        pbuf[...] = jnp.zeros_like(pbuf)
        pbuf[pl.ds(inner, ch), :] = total
        csend[j] = jnp.dot(
            p_out[:, pl.ds(base, span)], pbuf[...], precision=HI, preferred_element_type=F32
        )
        pl.when(t > 0)(lambda: c_copy(j).start())

    def loop(t):
        for s in range(1, nz):
            b = t - 1 - s
            pl.when((b >= 0) & (b < ns))(lambda b=b, s=s: line(block(b)).relay(s))
        pl.when(t < ns)(lambda: partial_stage(t))
        pl.when((t >= 1) & (t < ns + 1))(lambda: sum_stage(t - 1))
        pl.when(t < ns)(lambda: pair_stage(t))

    own_block.wait()
    partial_stage(0)
    pair_stage(0)
    each(1, nr, lambda t: probe_copy(t, lax.rem(row + t, nr)).wait_recv())
    probe = pvs[0]
    for k in range(1, nr):
        probe = probe + pvs[k]
    p_out[...] = probe
    each(1, ns + nz, loop)
    each(0, ns, lambda j: line(j).finish())

    w = ns * width // nr
    left = row * w // width
    if w < width:
        off = pl.multiple_of(lax.rem(row * w, width), w)
        part = s_out[left, :, :, pl.ds(off, w)]
    else:
        part = s_out[left]
    part = part.reshape(m, w).astype(F32).T.astype(BF16)

    def x_copy(t):
        to = lax.rem(me + t, ns)
        return remote(xsend.at[to], xs.at[me], xsnd.at[t], xrcv.at[me], "section", to)

    def gram_of(i):
        right = s_out[i].reshape(m, width)
        xsend[i] = jnp.dot(part, right, preferred_element_type=F32)

    def gram_stage(t):
        gram_of(lax.rem(me + t, ns))
        x_copy(t).start()

    each(1, ns, gram_stage)
    gram_of(me)

    def gather(t):
        i = lax.rem(me + t, ns)
        remote(xsend.at[i], xs.at[i], xsnd.at[0], xrcv.at[i], "section", i).wait_recv()
        remote(csend.at[i], cs.at[i], csnd.at[i], crcv.at[i], "section", i).wait_recv()

    each(1, ns, gather)
    xt, ct = xsend[me], csend[me]
    for t in range(1, ns):
        i = lax.rem(me + t, ns)
        xt = xt + xs[i]
        ct = ct + cs[i]
    cg[row] = ct
    x_out[row] = xt

    def k_copy(t, slot):
        return remote(
            cg.at[slot], cg.at[slot], ksend.at[t], krecv.at[slot], "row", lax.rem(row + t, nr)
        )

    each(1, nr, lambda t: k_copy(t, row).start())

    final = Line(
        z, nz, c, lambda core, slot: x_out.at[slot * 2 + core],
        lambda q: gup.at[q], lambda q: gdown.at[q], lambda q: grecv.at[q],
        lambda q: hsend.at[q], lambda q: hrecv.at[q],
    )
    final.begin()

    rows = b_out.shape[1]
    start = pl.multiple_of(me * rows, rows)
    b_out[...] = bg[:, pl.ds(start, rows), :]

    each(1, nz, final.relay)
    final.finish()
    each(1, nr, lambda t: k_copy(t, lax.rem(row + t, nr)).wait_recv())
    ct = cg[0]
    for k in range(1, nr):
        ct = ct + cg[k]
    c_out[...] = ct

    each(1, nr, lambda t: k_copy(t, row).wait_send())
    first_copy(rsend, rrecv, near(1)).wait_send()
    first_copy(lsend, lrecv, near(-1)).wait_send()
    for d in range(1, far):
        right_copy(d, d + 1 == far).wait_send()
        left_copy(d, d + 1 == far).wait_send()
    each(1, nr, lambda t: probe_copy(t, row).wait_send())

    def drain(j):
        pair_copy(j).wait_send()
        each(1, nz, lambda s: z_copy(j, s, z).wait_send())
        line(j).drain()

    each(0, ns, drain)
    each(1, ns, lambda t: x_copy(t).wait_send())
    each(1, ns, lambda t: c_copy(block(t)).wait_send())
    final.drain()


def invert_tile(mat):
    size = mat.shape[0]
    lane = lax.broadcasted_iota(jnp.int32, (size, size), 1)
    sub = lax.broadcasted_iota(jnp.int32, (PAD, size), 0)
    short = lax.broadcasted_iota(jnp.int32, (PAD, size), 1)
    for k in range(0, size, PAD):
        cols = [jnp.broadcast_to(mat[:, k + q:k + q + 1], (size, size)) for q in range(PAD)]
        heads = [col[k:k + PAD] for col in cols]
        rows = jnp.where((short >= k) & (short < k + PAD), 0.0, mat[k:k + PAD])
        rows = rows + jnp.where(short == sub + k, 1.0, 0.0)
        for p in range(PAD):
            scale = 1.0 / heads[p][p:p + 1]
            line = rows[p:p + 1] * scale
            rows = jnp.where(sub == p, line, rows - heads[p] * line)
            for q in range(p + 1, PAD):
                head = heads[q][p:p + 1] * scale
                heads[q] = jnp.where(sub == p, head, heads[q] - heads[p] * head)
        mat = jnp.where((lane >= k) & (lane < k + PAD), 0.0, mat)
        for q in range(PAD):
            mat = mat - cols[q] * rows[q:q + 1]
        parts = [mat[:k], rows, mat[k + PAD:]]
        mat = jnp.concatenate([part for part in parts if part.shape[0]], axis=0)
    return mat


def invert_kernel(x, inv):
    width = inv.shape[0]
    size = min(width, 128)
    inv[...] = x[lax.axis_index("section")]
    column = lax.broadcasted_iota(jnp.int32, (width, width), 1) // size
    eye = (
        lax.broadcasted_iota(jnp.int32, (size, size), 0)
        == lax.broadcasted_iota(jnp.int32, (size, size), 1)
    ).astype(F32)

    def step(b, carry):
        at = pl.ds(pl.multiple_of(b * size, size), size)
        pivot = invert_tile(inv[at, at])
        left = inv[:, at]
        inv[at, at] = eye
        rows = jnp.dot(pivot, inv[at, :], precision=HI, preferred_element_type=F32)
        rest = jnp.where(column == b, 0.0, inv[...])
        inv[...] = rest - jnp.dot(left, rows, precision=HI, preferred_element_type=F32)
        inv[at, :] = rows
        return carry

    lax.fori_loop(0, width // size, step, 0)


def solve_kernel(
    ns, n, x, inv, c0, s_in, p0, b, vec, ortho, coef,
    rbuf, cur, sm, rsend, rrecv, ssend, srecv,
):
    me = lax.axis_index("section")
    m, width = p0.shape[1], c0.shape[1]
    greet((("section", ns),))
    cur[...] = c0[...]

    def r_copy(t, slot):
        return remote(
            rbuf.at[slot], rbuf.at[slot], rsend.at[t], rrecv.at[slot],
            "section", lax.rem(me + t, ns),
        )

    def chain(j):
        @pl.when(me == j)
        def _():
            rbuf[me] = jnp.dot(cur[...], inv[...], precision=HI, preferred_element_type=F32)
            each(1, ns, lambda t: r_copy(t, me).start())

        @pl.when(me != j)
        def _():
            remote(rbuf.at[j], rbuf.at[j], rsend.at[0], rrecv.at[j], "section", j).wait_recv()

        @pl.when(me > j)
        def _():
            cur[...] -= jnp.dot(rbuf[j], x[j], precision=HI, preferred_element_type=F32)

    each(0, ns, chain)

    def fold(j, carry):
        probe, remain = carry
        r = rbuf[j]
        sj = s_in[j].reshape(m, width).astype(F32)
        nt = (((1,), (1,)), ((), ()))
        probe = probe - lax.dot_general(r, sj, nt, precision=HI, preferred_element_type=F32)
        rb = jnp.concatenate([r, r], axis=0).astype(BF16)
        remain = remain - lax.dot_general(rb, b[j], nt, preferred_element_type=F32)[:PAD]
        return probe, remain

    probe, remain = lax.fori_loop(0, ns, fold, (p0[...], vec[...]))
    small = lax.dot_general(
        probe, probe, (((1,), (1,)), ((), ())), precision=HI, preferred_element_type=F32
    )
    sm[me] = jnp.concatenate([small, jnp.zeros((PAD, 128 - PAD), F32)], axis=1)

    def s_copy(t, slot):
        return remote(
            sm.at[slot], sm.at[slot], ssend.at[t], srecv.at[slot],
            "section", lax.rem(me + t, ns),
        )

    each(1, ns, lambda t: s_copy(t, me).start())
    coef[...] = rbuf[me, :n]
    each(1, ns, lambda t: s_copy(t, lax.rem(me + t, ns)).wait_recv())
    full = sm[0]
    for k in range(1, ns):
        full = full + sm[k]
    low = {}
    rows = []
    for i in range(n):
        for k in range(i + 1):
            value = full[i:i + 1, k:k + 1]
            for q in range(k):
                value = value - low[i, q] * low[k, q]
            low[i, k] = jnp.sqrt(value) if i == k else value / low[k, k]
        line = remain[i:i + 1]
        for k in range(i):
            line = line - low[i, k] * rows[k]
        rows.append(line / low[i, i])
        ortho[i:i + 1, :] = rows[i]
    each(1, ns, lambda t: r_copy(t, me).wait_send())
    each(1, ns, lambda t: s_copy(t, me).wait_send())


def body(ns, nr, omega, basis, vectors):
    dma = pltpu.SemaphoreType.DMA
    n, k = vectors.shape
    m, width = omega.shape[0], basis.shape[1]
    nz = nr // 2
    half = m // 2
    ch = half // nz
    w = ns * width // nr
    rows = k // ns
    vmem = pl.BlockSpec(memory_space=pltpu.VMEM)
    padded = jnp.pad(vectors, ((0, 2 * PAD - n), (0, 0)))
    s_all, x, c0, p0, b = pl.pallas_call(
        functools.partial(sketch_kernel, ns, nr),
        out_shape=(
            jax.ShapeDtypeStruct((ns, nr, ch, width), BF16),
            jax.ShapeDtypeStruct((nr, w, width), F32),
            jax.ShapeDtypeStruct((PAD, width), F32),
            jax.ShapeDtypeStruct((PAD, m), F32),
            jax.ShapeDtypeStruct((ns, rows, width), BF16),
        ),
        in_specs=[vmem] * 3,
        out_specs=(vmem,) * 5,
        scratch_shapes=[
            pltpu.VMEM((ns, k, width), BF16),
            pltpu.VMEM((ns, m, width), F32),
            pltpu.VMEM((ns, half, width), F32),
            pltpu.VMEM((ns, nz, ch, width), F32),
            pltpu.VMEM((ns, nz, ch, width), F32),
            pltpu.VMEM((ns, w, width), F32),
            pltpu.VMEM((ns, w, width), F32),
            pltpu.VMEM((ns, PAD, width), F32),
            pltpu.VMEM((ns, PAD, width), F32),
            pltpu.VMEM((nr, PAD, m), F32),
            pltpu.VMEM((max(ch, 128), width), F32),
            pltpu.VMEM((nr, PAD, width), F32),
            dma((ns,)), dma((ns,)), dma((ns,)), dma((ns,)), dma((nr,)), dma((nr,)),
            dma((ns,)), dma((ns,)), dma((ns, nz)), dma((ns, nz)),
            dma((ns, nz)), dma((ns, nz)), dma((ns, nz)), dma((ns, nz)), dma((ns, nz)),
            dma((ns,)), dma((ns,)), dma((ns,)), dma((ns,)),
            dma((nz,)), dma((nz,)), dma((nz,)), dma((nz,)), dma((nz,)), dma((nr,)), dma((nr,)),
            dma,
        ],
        compiler_params=pltpu.CompilerParams(
            collective_id=0, has_side_effects=True, vmem_limit_bytes=60 * 2**20
        ),
    )(omega, basis, padded)
    x = x.reshape(ns, width, width)
    me = lax.axis_index("section")
    inv = pl.pallas_call(
        invert_kernel,
        out_shape=jax.ShapeDtypeStruct((width, width), F32),
        in_specs=[vmem],
        out_specs=vmem,
        compiler_params=pltpu.CompilerParams(vmem_limit_bytes=32 * 2**20),
    )(x)
    mine = lax.dynamic_slice_in_dim(vectors, me * rows, rows, 1).astype(F32)
    mine = jnp.pad(mine, ((0, PAD - n), (0, 0)))
    return pl.pallas_call(
        functools.partial(solve_kernel, ns, n),
        out_shape=(
            jax.ShapeDtypeStruct((n, rows), F32),
            jax.ShapeDtypeStruct((n, width), F32),
        ),
        in_specs=[vmem] * 7,
        out_specs=(vmem,) * 2,
        scratch_shapes=[
            pltpu.VMEM((ns, PAD, width), F32),
            pltpu.VMEM((PAD, width), F32),
            pltpu.VMEM((ns, PAD, 128), F32),
            dma((ns,)), dma((ns,)), dma((ns,)), dma((ns,)),
        ],
        compiler_params=pltpu.CompilerParams(
            collective_id=1, has_side_effects=True, vmem_limit_bytes=60 * 2**20
        ),
    )(x, inv, c0, s_all, p0, b, mine)


def solution(mesh):
    return jax.shard_map(
        functools.partial(body, mesh.shape["section"], mesh.shape["row"]),
        mesh=mesh,
        in_specs=(P("section", "row"), P("row", "section"), P(None, "row")),
        out_specs=(P(None, ("row", "section")), P(None, "section")),
        check_vma=False,
    )
```

```python
import functools

import jax
import jax.numpy as jnp
from jax import lax
from jax.experimental import pallas as pl
from jax.experimental.pallas import tpu as pltpu
from jax.sharding import PartitionSpec as P

MESH = pl.DeviceIdType.MESH
HI = lax.Precision.HIGHEST
F32 = jnp.float32
BF16 = jnp.bfloat16
PAD = 8


def remote(src, dst, send, recv, axis, index):
    return pltpu.make_async_remote_copy(
        src_ref=src, dst_ref=dst, send_sem=send, recv_sem=recv,
        device_id={axis: index}, device_id_type=MESH,
    )


def each(first, count, fn):
    def step(t, carry):
        fn(t)
        return carry

    lax.fori_loop(first, count, step, 0)


def greet(pairs):
    barrier = pltpu.get_barrier_semaphore()
    total = 0
    for axis, count in pairs:
        me = lax.axis_index(axis)

        def hello(t, axis=axis, count=count, me=me):
            pl.semaphore_signal(
                barrier, inc=1, device_id={axis: lax.rem(me + t, count)}, device_id_type=MESH
            )

        each(1, count, hello)
        total += count - 1
    pl.semaphore_wait(barrier, total)


class Line:
    def __init__(self, z, nz, c, chunk, up, down, recv, fsend, frecv):
        self.z, self.nz, self.c, self.chunk = z, nz, c, chunk
        self.up, self.down, self.recv = up, down, recv
        self.fsend, self.frecv = fsend, frecv

    def rise(self, slot):
        piece = self.chunk(self.c, slot)
        to = (self.z + 1) * 2 + self.c
        return remote(piece, piece, self.up(slot), self.recv(slot), "row", to)

    def sink(self, slot):
        piece = self.chunk(self.c, slot)
        to = (self.z - 1) * 2 + self.c
        return remote(piece, piece, self.down(slot), self.recv(slot), "row", to)

    def across(self, core, slot):
        piece = self.chunk(core, slot)
        to = self.z * 2 + 1 - self.c
        return remote(piece, piece, self.fsend(slot), self.frecv(slot), "row", to)

    def send(self, slot, upward, downward):
        if upward:
            pl.when(self.z < self.nz - 1)(lambda: self.rise(slot).start())
        if downward:
            pl.when(self.z > 0)(lambda: self.sink(slot).start())
        self.across(self.c, slot).start()

    def begin(self):
        self.send(self.z, True, True)

    def relay(self, s):
        @pl.when(self.z >= s)
        def _():
            self.sink(self.z - s).wait_recv()
            self.send(self.z - s, True, False)

        @pl.when(self.z + s < self.nz)
        def _():
            self.sink(self.z + s).wait_recv()
            self.send(self.z + s, False, True)

    def finish(self):
        each(0, self.nz, lambda q: self.across(1 - self.c, q).wait_recv())

    def drain(self):
        def one(q):
            pl.when((q <= self.z) & (self.z < self.nz - 1))(lambda: self.rise(q).wait_send())
            pl.when((q >= self.z) & (self.z > 0))(lambda: self.sink(q).wait_send())
            self.across(self.c, q).wait_send()

        each(0, self.nz, one)


def sketch_kernel(
    ns, nr, omega, basis, vec, s_out, x_out, c_out, p_out, b_out,
    bg, acc, pslot, hs, zslot, xs, xsend, cs, csend, pvs, pbuf, cg,
    rsend, rrecv, lsend, lrecv, psend, precv, qsend, qrecv, zsend, zrecv,
    aup, adown, arecv, fsend, frecv, xsnd, xrcv, csnd, crcv,
    gup, gdown, grecv, hsend, hrecv, ksend, krecv, lbsem,
):
    me = lax.axis_index("section")
    row = lax.axis_index("row")
    nz = nr // 2
    z, c = row // 2, lax.rem(row, 2)
    partner = z * 2 + 1 - c
    m, width = omega.shape[0], basis.shape[1]
    half = m // 2
    ch = half // nz
    span = pbuf.shape[0]
    mine = c * nz + z
    greet((("section", ns), ("row", nr)))

    far = ns // 2
    tall = basis.shape[0] // 2

    def at_place(p):
        return jnp.where(p < far, p, ns + far - 1 - p)

    place = at_place(me)

    def near(d):
        return at_place(lax.rem(place + d + ns, ns))

    def right_copy(d, part):
        origin = near(-d)
        block = bg.at[origin, pl.ds(0, tall)] if part else bg.at[origin]
        return remote(block, block, rsend.at[d], rrecv.at[origin], "section", near(1))

    def left_copy(d, part):
        origin = near(d)
        block = bg.at[origin, pl.ds(tall, tall)] if part else bg.at[origin]
        return remote(block, block, lsend.at[d], lrecv.at[origin], "section", near(-1))

    def first_copy(send, recv, to):
        return remote(basis, bg.at[me], send.at[0], recv.at[me], "section", to)

    first_copy(rsend, rrecv, near(1)).start()
    first_copy(lsend, lrecv, near(-1)).start()
    own_block = pltpu.make_async_copy(basis, bg.at[me], lbsem)
    own_block.start()
    pvs[row] = lax.dot_general(
        vec[...], omega[...], (((1,), (1,)), ((), ())), preferred_element_type=F32
    )[:PAD]

    def probe_copy(t, slot):
        return remote(
            pvs.at[slot], pvs.at[slot], psend.at[t], precv.at[slot], "row", lax.rem(row + t, nr)
        )

    each(1, nr, lambda t: probe_copy(t, row).start())

    def pair_copy(j):
        other = pl.multiple_of((1 - c) * half, half)
        return remote(
            acc.at[j, pl.ds(other, half)], pslot.at[j], qsend.at[j], qrecv.at[j], "row", partner
        )

    def z_copy(j, t, slot):
        to = lax.rem(z + t, nz)
        return remote(
            hs.at[j, to], zslot.at[j, slot], zsend.at[j, t], zrecv.at[j, slot], "row", to * 2 + c
        )

    def line(j):
        return Line(
            z, nz, c, lambda core, slot: s_out.at[j, core * nz + slot],
            lambda q: aup.at[j, q], lambda q: adown.at[j, q], lambda q: arecv.at[j, q],
            lambda q: fsend.at[j, q], lambda q: frecv.at[j, q],
        )

    def c_copy(j):
        return remote(csend.at[j], cs.at[me], csnd.at[j], crcv.at[me], "section", j)

    def block(t):
        d = (t + 1) // 2
        return near(jnp.where(lax.rem(t, 2) == 1, ns - d, d))

    def arrive(d):
        @pl.when(d < far)
        def _():
            right_copy(d, False).wait_recv()
            left_copy(d, False).wait_recv()

            @pl.when(d + 1 < far)
            def _():
                right_copy(d, False).start()
                left_copy(d, False).start()

            @pl.when(d + 1 == far)
            def _():
                right_copy(d, True).start()
                left_copy(d, True).start()

        @pl.when(d == far)
        def _():
            right_copy(far, True).wait_recv()
            left_copy(far, True).wait_recv()

    def partial_stage(t):
        j = block(t)
        pl.when(lax.rem(t, 2) == 1)(lambda: arrive((t + 1) // 2))
        acc[j] = jnp.dot(omega[...], bg[j], preferred_element_type=F32)
        pair_copy(j).start()

    def pair_stage(t):
        j = block(t)
        pair_copy(j).wait_recv()
        own = pl.multiple_of(c * half, half)
        total = acc[j, pl.ds(own, half)] + pslot[j]
        pslot[j] = total
        hs[j] = total.reshape(nz, ch, width)
        each(1, nz, lambda s: z_copy(j, s, z).start())

    def sum_stage(t):
        j = block(t)
        each(1, nz, lambda s: z_copy(j, s, lax.rem(z + s, nz)).wait_recv())
        total = pslot[j, pl.ds(pl.multiple_of(z * ch, ch), ch)]
        for s in range(1, nz):
            total = total + zslot[j, lax.rem(z + s, nz)]
        s_out[j, mine] = total.astype(BF16)
        line(j).begin()
        first = mine * ch
        base = pl.multiple_of(first // span * span, span)
        inner = pl.multiple_of(lax.rem(first, span), ch)
        pbuf[...] = jnp.zeros_like(pbuf)
        pbuf[pl.ds(inner, ch), :] = total
        csend[j] = jnp.dot(
            p_out[:, pl.ds(base, span)], pbuf[...], precision=HI, preferred_element_type=F32
        )
        pl.when(t > 0)(lambda: c_copy(j).start())

    def loop(t):
        for s in range(1, nz):
            b = t - 1 - s
            pl.when((b >= 0) & (b < ns))(lambda b=b, s=s: line(block(b)).relay(s))
        pl.when(t < ns)(lambda: partial_stage(t))
        pl.when((t >= 1) & (t < ns + 1))(lambda: sum_stage(t - 1))
        pl.when(t < ns)(lambda: pair_stage(t))

    own_block.wait()
    partial_stage(0)
    pair_stage(0)
    each(1, nr, lambda t: probe_copy(t, lax.rem(row + t, nr)).wait_recv())
    probe = pvs[0]
    for k in range(1, nr):
        probe = probe + pvs[k]
    p_out[...] = probe
    each(1, ns + nz, loop)
    each(0, ns, lambda j: line(j).finish())

    w = ns * width // nr
    left = row * w // width
    if w < width:
        off = pl.multiple_of(lax.rem(row * w, width), w)
        part = s_out[left, :, :, pl.ds(off, w)]
    else:
        part = s_out[left]
    part = part.reshape(m, w).astype(F32).T.astype(BF16)

    def x_copy(t):
        to = lax.rem(me + t, ns)
        return remote(xsend.at[to], xs.at[me], xsnd.at[t], xrcv.at[me], "section", to)

    def gram_of(i):
        right = s_out[i].reshape(m, width)
        xsend[i] = jnp.dot(part, right, preferred_element_type=F32)

    def gram_stage(t):
        gram_of(lax.rem(me + t, ns))
        x_copy(t).start()

    each(1, ns, gram_stage)
    gram_of(me)

    def gather(t):
        i = lax.rem(me + t, ns)
        remote(xsend.at[i], xs.at[i], xsnd.at[0], xrcv.at[i], "section", i).wait_recv()
        remote(csend.at[i], cs.at[i], csnd.at[i], crcv.at[i], "section", i).wait_recv()

    each(1, ns, gather)
    xt, ct = xsend[me], csend[me]
    for t in range(1, ns):
        i = lax.rem(me + t, ns)
        xt = xt + xs[i]
        ct = ct + cs[i]
    cg[row] = ct
    x_out[row] = xt

    def k_copy(t, slot):
        return remote(
            cg.at[slot], cg.at[slot], ksend.at[t], krecv.at[slot], "row", lax.rem(row + t, nr)
        )

    each(1, nr, lambda t: k_copy(t, row).start())

    deep = w // 2

    def final(h):
        return Line(
            z, nz, c, lambda core, slot: x_out.at[slot * 2 + core, pl.ds(h * deep, deep)],
            lambda q: gup.at[h, q], lambda q: gdown.at[h, q], lambda q: grecv.at[h, q],
            lambda q: hsend.at[h, q], lambda q: hrecv.at[h, q],
        )

    each(0, 2, lambda h: final(h).begin())

    rows = b_out.shape[1]
    start = pl.multiple_of(me * rows, rows)
    b_out[...] = bg[:, pl.ds(start, rows), :]

    each(1, nz, lambda s: each(0, 2, lambda h: final(h).relay(s)))
    each(0, 2, lambda h: final(h).finish())
    each(1, nr, lambda t: k_copy(t, lax.rem(row + t, nr)).wait_recv())
    ct = cg[0]
    for k in range(1, nr):
        ct = ct + cg[k]
    c_out[...] = ct

    each(1, nr, lambda t: k_copy(t, row).wait_send())
    first_copy(rsend, rrecv, near(1)).wait_send()
    first_copy(lsend, lrecv, near(-1)).wait_send()
    for d in range(1, far):
        right_copy(d, d + 1 == far).wait_send()
        left_copy(d, d + 1 == far).wait_send()
    each(1, nr, lambda t: probe_copy(t, row).wait_send())

    def drain(j):
        pair_copy(j).wait_send()
        each(1, nz, lambda s: z_copy(j, s, z).wait_send())
        line(j).drain()

    each(0, ns, drain)
    each(1, ns, lambda t: x_copy(t).wait_send())
    each(1, ns, lambda t: c_copy(block(t)).wait_send())
    each(0, 2, lambda h: final(h).drain())


def invert_tile(mat):
    size = mat.shape[0]
    lane = lax.broadcasted_iota(jnp.int32, (size, size), 1)
    sub = lax.broadcasted_iota(jnp.int32, (PAD, size), 0)
    short = lax.broadcasted_iota(jnp.int32, (PAD, size), 1)
    for k in range(0, size, PAD):
        cols = [jnp.broadcast_to(mat[:, k + q:k + q + 1], (size, size)) for q in range(PAD)]
        heads = [col[k:k + PAD] for col in cols]
        rows = jnp.where((short >= k) & (short < k + PAD), 0.0, mat[k:k + PAD])
        rows = rows + jnp.where(short == sub + k, 1.0, 0.0)
        for p in range(PAD):
            scale = 1.0 / heads[p][p:p + 1]
            line = rows[p:p + 1] * scale
            rows = jnp.where(sub == p, line, rows - heads[p] * line)
            for q in range(p + 1, PAD):
                head = heads[q][p:p + 1] * scale
                heads[q] = jnp.where(sub == p, head, heads[q] - heads[p] * head)
        mat = jnp.where((lane >= k) & (lane < k + PAD), 0.0, mat)
        for q in range(PAD):
            mat = mat - cols[q] * rows[q:q + 1]
        parts = [mat[:k], rows, mat[k + PAD:]]
        mat = jnp.concatenate([part for part in parts if part.shape[0]], axis=0)
    return mat


def invert_kernel(x, inv):
    width = inv.shape[0]
    size = min(width, 128)
    inv[...] = x[lax.axis_index("section")]
    column = lax.broadcasted_iota(jnp.int32, (width, width), 1) // size
    eye = (
        lax.broadcasted_iota(jnp.int32, (size, size), 0)
        == lax.broadcasted_iota(jnp.int32, (size, size), 1)
    ).astype(F32)

    def step(b, carry):
        at = pl.ds(pl.multiple_of(b * size, size), size)
        pivot = invert_tile(inv[at, at])
        left = inv[:, at]
        inv[at, at] = eye
        rows = jnp.dot(pivot, inv[at, :], precision=HI, preferred_element_type=F32)
        rest = jnp.where(column == b, 0.0, inv[...])
        inv[...] = rest - jnp.dot(left, rows, precision=HI, preferred_element_type=F32)
        inv[at, :] = rows
        return carry

    lax.fori_loop(0, width // size, step, 0)


def solve_kernel(
    ns, n, x, inv, c0, s_in, p0, b, vec, ortho, coef,
    rbuf, cur, probe_ref, remain_ref, sm, rsend, rrecv, ssend, srecv,
):
    me = lax.axis_index("section")
    m, width = p0.shape[1], c0.shape[1]
    greet((("section", ns),))
    cur[...] = c0[...]

    def r_copy(t, slot):
        return remote(
            rbuf.at[slot], rbuf.at[slot], rsend.at[t], rrecv.at[slot],
            "section", lax.rem(me + t, ns),
        )

    nt = (((1,), (1,)), ((), ()))
    probe_ref[...] = p0[...]
    remain_ref[...] = vec[...]

    def fold(j):
        r = rbuf[j]
        high = r.astype(BF16).astype(F32)
        mid = (r - high).astype(BF16).astype(F32)
        low = r - high - mid
        parts = jnp.concatenate([high, mid, low, jnp.zeros_like(r)], axis=0).astype(BF16)
        moved = lax.dot_general(
            parts, s_in[j].reshape(m, width), nt, preferred_element_type=F32
        )
        probe_ref[...] -= moved[:PAD] + (moved[PAD:2 * PAD] + moved[2 * PAD:3 * PAD])
        taken = lax.dot_general(parts[:2 * PAD], b[j], nt, preferred_element_type=F32)
        remain_ref[...] -= taken[:PAD]

    def chain(j):
        @pl.when(me == j)
        def _():
            rbuf[me] = jnp.dot(cur[...], inv[...], precision=HI, preferred_element_type=F32)
            each(1, ns, lambda t: r_copy(t, me).start())

        pl.when(j > 0)(lambda: fold(j - 1))

        @pl.when(me != j)
        def _():
            remote(rbuf.at[j], rbuf.at[j], rsend.at[0], rrecv.at[j], "section", j).wait_recv()

        @pl.when(me > j)
        def _():
            cur[...] -= jnp.dot(rbuf[j], x[j], precision=HI, preferred_element_type=F32)

    each(0, ns, chain)
    fold(ns - 1)
    probe, remain = probe_ref[...], remain_ref[...]
    small = lax.dot_general(
        probe, probe, (((1,), (1,)), ((), ())), precision=HI, preferred_element_type=F32
    )
    sm[me] = jnp.concatenate([small, jnp.zeros((PAD, 128 - PAD), F32)], axis=1)

    def s_copy(t, slot):
        return remote(
            sm.at[slot], sm.at[slot], ssend.at[t], srecv.at[slot],
            "section", lax.rem(me + t, ns),
        )

    each(1, ns, lambda t: s_copy(t, me).start())
    coef[...] = rbuf[me, :n]
    each(1, ns, lambda t: s_copy(t, lax.rem(me + t, ns)).wait_recv())
    full = sm[0]
    for k in range(1, ns):
        full = full + sm[k]
    low = {}
    rows = []
    for i in range(n):
        for k in range(i + 1):
            value = full[i:i + 1, k:k + 1]
            for q in range(k):
                value = value - low[i, q] * low[k, q]
            low[i, k] = jnp.sqrt(value) if i == k else value / low[k, k]
        line = remain[i:i + 1]
        for k in range(i):
            line = line - low[i, k] * rows[k]
        rows.append(line / low[i, i])
        ortho[i:i + 1, :] = rows[i]
    each(1, ns, lambda t: r_copy(t, me).wait_send())
    each(1, ns, lambda t: s_copy(t, me).wait_send())


def body(ns, nr, omega, basis, vectors):
    dma = pltpu.SemaphoreType.DMA
    n, k = vectors.shape
    m, width = omega.shape[0], basis.shape[1]
    nz = nr // 2
    half = m // 2
    ch = half // nz
    w = ns * width // nr
    rows = k // ns
    vmem = pl.BlockSpec(memory_space=pltpu.VMEM)
    padded = jnp.pad(vectors, ((0, 2 * PAD - n), (0, 0)))
    s_all, x, c0, p0, b = pl.pallas_call(
        functools.partial(sketch_kernel, ns, nr),
        out_shape=(
            jax.ShapeDtypeStruct((ns, nr, ch, width), BF16),
            jax.ShapeDtypeStruct((nr, w, width), F32),
            jax.ShapeDtypeStruct((PAD, width), F32),
            jax.ShapeDtypeStruct((PAD, m), F32),
            jax.ShapeDtypeStruct((ns, rows, width), BF16),
        ),
        in_specs=[vmem] * 3,
        out_specs=(vmem,) * 5,
        scratch_shapes=[
            pltpu.VMEM((ns, k, width), BF16),
            pltpu.VMEM((ns, m, width), F32),
            pltpu.VMEM((ns, half, width), F32),
            pltpu.VMEM((ns, nz, ch, width), F32),
            pltpu.VMEM((ns, nz, ch, width), F32),
            pltpu.VMEM((ns, w, width), F32),
            pltpu.VMEM((ns, w, width), F32),
            pltpu.VMEM((ns, PAD, width), F32),
            pltpu.VMEM((ns, PAD, width), F32),
            pltpu.VMEM((nr, PAD, m), F32),
            pltpu.VMEM((max(ch, 128), width), F32),
            pltpu.VMEM((nr, PAD, width), F32),
            dma((ns,)), dma((ns,)), dma((ns,)), dma((ns,)), dma((nr,)), dma((nr,)),
            dma((ns,)), dma((ns,)), dma((ns, nz)), dma((ns, nz)),
            dma((ns, nz)), dma((ns, nz)), dma((ns, nz)), dma((ns, nz)), dma((ns, nz)),
            dma((ns,)), dma((ns,)), dma((ns,)), dma((ns,)),
            dma((2, nz)), dma((2, nz)), dma((2, nz)), dma((2, nz)), dma((2, nz)),
            dma((nr,)), dma((nr,)),
            dma,
        ],
        compiler_params=pltpu.CompilerParams(
            collective_id=0, has_side_effects=True, vmem_limit_bytes=60 * 2**20
        ),
    )(omega, basis, padded)
    x = x.reshape(ns, width, width)
    me = lax.axis_index("section")
    inv = pl.pallas_call(
        invert_kernel,
        out_shape=jax.ShapeDtypeStruct((width, width), F32),
        in_specs=[vmem],
        out_specs=vmem,
        compiler_params=pltpu.CompilerParams(vmem_limit_bytes=32 * 2**20),
    )(x)
    mine = lax.dynamic_slice_in_dim(vectors, me * rows, rows, 1).astype(F32)
    mine = jnp.pad(mine, ((0, PAD - n), (0, 0)))
    return pl.pallas_call(
        functools.partial(solve_kernel, ns, n),
        out_shape=(
            jax.ShapeDtypeStruct((n, rows), F32),
            jax.ShapeDtypeStruct((n, width), F32),
        ),
        in_specs=[vmem] * 7,
        out_specs=(vmem,) * 2,
        scratch_shapes=[
            pltpu.VMEM((ns, PAD, width), F32),
            pltpu.VMEM((PAD, width), F32),
            pltpu.VMEM((PAD, m), F32),
            pltpu.VMEM((PAD, rows), F32),
            pltpu.VMEM((ns, PAD, 128), F32),
            dma((ns,)), dma((ns,)), dma((ns,)), dma((ns,)),
        ],
        compiler_params=pltpu.CompilerParams(
            collective_id=1, has_side_effects=True, vmem_limit_bytes=60 * 2**20
        ),
    )(x, inv, c0, s_all, p0, b, mine)


def solution(mesh):
    return jax.shard_map(
        functools.partial(body, mesh.shape["section"], mesh.shape["row"]),
        mesh=mesh,
        in_specs=(P("section", "row"), P("row", "section"), P(None, "row")),
        out_specs=(P(None, ("row", "section")), P(None, "section")),
        check_vma=False,
    )
```

```python
import functools

import jax
import jax.numpy as jnp
from jax import lax
from jax.experimental import pallas as pl
from jax.experimental.pallas import tpu as pltpu
from jax.sharding import PartitionSpec as P

MESH = pl.DeviceIdType.MESH
HI = lax.Precision.HIGHEST
F32 = jnp.float32
BF16 = jnp.bfloat16
PAD = 8


def remote(src, dst, send, recv, axis, index):
    return pltpu.make_async_remote_copy(
        src_ref=src, dst_ref=dst, send_sem=send, recv_sem=recv,
        device_id={axis: index}, device_id_type=MESH,
    )


def each(first, count, fn):
    def step(t, carry):
        fn(t)
        return carry

    lax.fori_loop(first, count, step, 0)


def greet(pairs):
    barrier = pltpu.get_barrier_semaphore()
    total = 0
    for axis, count in pairs:
        me = lax.axis_index(axis)

        def hello(t, axis=axis, count=count, me=me):
            pl.semaphore_signal(
                barrier, inc=1, device_id={axis: lax.rem(me + t, count)}, device_id_type=MESH
            )

        each(1, count, hello)
        total += count - 1
    pl.semaphore_wait(barrier, total)


class Line:
    def __init__(self, z, nz, c, chunk, up, down, recv, fsend, frecv):
        self.z, self.nz, self.c, self.chunk = z, nz, c, chunk
        self.up, self.down, self.recv = up, down, recv
        self.fsend, self.frecv = fsend, frecv

    def rise(self, slot):
        piece = self.chunk(self.c, slot)
        to = (self.z + 1) * 2 + self.c
        return remote(piece, piece, self.up(slot), self.recv(slot), "row", to)

    def sink(self, slot):
        piece = self.chunk(self.c, slot)
        to = (self.z - 1) * 2 + self.c
        return remote(piece, piece, self.down(slot), self.recv(slot), "row", to)

    def across(self, core, slot):
        piece = self.chunk(core, slot)
        to = self.z * 2 + 1 - self.c
        return remote(piece, piece, self.fsend(slot), self.frecv(slot), "row", to)

    def send(self, slot, upward, downward):
        if upward:
            pl.when(self.z < self.nz - 1)(lambda: self.rise(slot).start())
        if downward:
            pl.when(self.z > 0)(lambda: self.sink(slot).start())
        self.across(self.c, slot).start()

    def begin(self):
        self.send(self.z, True, True)

    def relay(self, s):
        @pl.when(self.z >= s)
        def _():
            self.sink(self.z - s).wait_recv()
            self.send(self.z - s, True, False)

        @pl.when(self.z + s < self.nz)
        def _():
            self.sink(self.z + s).wait_recv()
            self.send(self.z + s, False, True)

    def finish(self):
        each(0, self.nz, lambda q: self.across(1 - self.c, q).wait_recv())

    def drain(self):
        def one(q):
            pl.when((q <= self.z) & (self.z < self.nz - 1))(lambda: self.rise(q).wait_send())
            pl.when((q >= self.z) & (self.z > 0))(lambda: self.sink(q).wait_send())
            self.across(self.c, q).wait_send()

        each(0, self.nz, one)


def sketch_kernel(
    ns, nr, omega, basis, vec, s_out, x_out, c_out, p_out, b_out, g_out,
    bg, acc, pslot, hs, zslot, xs, xsend, cs, csend, pvs, pbuf, cg,
    rsend, rrecv, lsend, lrecv, psend, precv, qsend, qrecv, zsend, zrecv,
    aup, adown, arecv, fsend, frecv, xsnd, xrcv, csnd, crcv,
    gup, gdown, grecv, hsend, hrecv, ksend, krecv, lbsem,
):
    me = lax.axis_index("section")
    row = lax.axis_index("row")
    nz = nr // 2
    z, c = row // 2, lax.rem(row, 2)
    partner = z * 2 + 1 - c
    m, width = omega.shape[0], basis.shape[1]
    half = m // 2
    ch = half // nz
    span = pbuf.shape[0]
    mine = c * nz + z
    greet((("section", ns), ("row", nr)))

    far = ns // 2
    tall = basis.shape[0] // 2

    def at_place(p):
        return jnp.where(p < far, p, ns + far - 1 - p)

    place = at_place(me)

    def near(d):
        return at_place(lax.rem(place + d + ns, ns))

    def right_copy(d, part):
        origin = near(-d)
        block = bg.at[origin, pl.ds(0, tall)] if part else bg.at[origin]
        return remote(block, block, rsend.at[d], rrecv.at[origin], "section", near(1))

    def left_copy(d, part):
        origin = near(d)
        block = bg.at[origin, pl.ds(tall, tall)] if part else bg.at[origin]
        return remote(block, block, lsend.at[d], lrecv.at[origin], "section", near(-1))

    def first_copy(send, recv, to):
        return remote(basis, bg.at[me], send.at[0], recv.at[me], "section", to)

    first_copy(rsend, rrecv, near(1)).start()
    first_copy(lsend, lrecv, near(-1)).start()
    own_block = pltpu.make_async_copy(basis, bg.at[me], lbsem)
    own_block.start()
    pvs[row] = lax.dot_general(
        vec[...], omega[...], (((1,), (1,)), ((), ())), preferred_element_type=F32
    )[:PAD]

    def probe_copy(t, slot):
        return remote(
            pvs.at[slot], pvs.at[slot], psend.at[t], precv.at[slot], "row", lax.rem(row + t, nr)
        )

    each(1, nr, lambda t: probe_copy(t, row).start())

    def pair_copy(j):
        other = pl.multiple_of((1 - c) * half, half)
        return remote(
            acc.at[j, pl.ds(other, half)], pslot.at[j], qsend.at[j], qrecv.at[j], "row", partner
        )

    def z_copy(j, t, slot):
        to = lax.rem(z + t, nz)
        return remote(
            hs.at[j, to], zslot.at[j, slot], zsend.at[j, t], zrecv.at[j, slot], "row", to * 2 + c
        )

    def line(j):
        return Line(
            z, nz, c, lambda core, slot: s_out.at[j, core * nz + slot],
            lambda q: aup.at[j, q], lambda q: adown.at[j, q], lambda q: arecv.at[j, q],
            lambda q: fsend.at[j, q], lambda q: frecv.at[j, q],
        )

    def c_copy(j):
        return remote(csend.at[j], cs.at[me], csnd.at[j], crcv.at[me], "section", j)

    def block(t):
        d = (t + 1) // 2
        return near(jnp.where(lax.rem(t, 2) == 1, ns - d, d))

    def arrive(d):
        @pl.when(d < far)
        def _():
            right_copy(d, False).wait_recv()
            left_copy(d, False).wait_recv()

            @pl.when(d + 1 < far)
            def _():
                right_copy(d, False).start()
                left_copy(d, False).start()

            @pl.when(d + 1 == far)
            def _():
                right_copy(d, True).start()
                left_copy(d, True).start()

        @pl.when(d == far)
        def _():
            right_copy(far, True).wait_recv()
            left_copy(far, True).wait_recv()

    def partial_stage(t):
        j = block(t)
        pl.when(lax.rem(t, 2) == 1)(lambda: arrive((t + 1) // 2))
        acc[j] = jnp.dot(omega[...], bg[j], preferred_element_type=F32)
        pair_copy(j).start()

    def pair_stage(t):
        j = block(t)
        pair_copy(j).wait_recv()
        own = pl.multiple_of(c * half, half)
        total = acc[j, pl.ds(own, half)] + pslot[j]
        pslot[j] = total
        hs[j] = total.reshape(nz, ch, width)
        each(1, nz, lambda s: z_copy(j, s, z).start())

    def sum_stage(t):
        j = block(t)
        each(1, nz, lambda s: z_copy(j, s, lax.rem(z + s, nz)).wait_recv())
        total = pslot[j, pl.ds(pl.multiple_of(z * ch, ch), ch)]
        for s in range(1, nz):
            total = total + zslot[j, lax.rem(z + s, nz)]
        s_out[j, mine] = total.astype(BF16)
        line(j).begin()
        first = mine * ch
        base = pl.multiple_of(first // span * span, span)
        inner = pl.multiple_of(lax.rem(first, span), ch)
        pbuf[...] = jnp.zeros_like(pbuf)
        pbuf[pl.ds(inner, ch), :] = total
        csend[j] = jnp.dot(
            p_out[:, pl.ds(base, span)], pbuf[...], precision=HI, preferred_element_type=F32
        )
        pl.when(t > 0)(lambda: c_copy(j).start())

    def loop(t):
        for s in range(1, nz):
            b = t - 1 - s
            pl.when((b >= 0) & (b < ns))(lambda b=b, s=s: line(block(b)).relay(s))
        pl.when(t < ns)(lambda: partial_stage(t))
        pl.when((t >= 1) & (t < ns + 1))(lambda: sum_stage(t - 1))
        pl.when(t < ns)(lambda: pair_stage(t))

    own_block.wait()
    partial_stage(0)
    pair_stage(0)
    each(1, nr, lambda t: probe_copy(t, lax.rem(row + t, nr)).wait_recv())
    probe = pvs[0]
    for k in range(1, nr):
        probe = probe + pvs[k]
    p_out[...] = probe
    each(1, ns + nz, loop)
    each(0, ns, lambda j: line(j).finish())

    w = ns * width // nr
    left = row * w // width
    if w < width:
        off = pl.multiple_of(lax.rem(row * w, width), w)
        part = s_out[left, :, :, pl.ds(off, w)]
    else:
        part = s_out[left]
    part = part.reshape(m, w).astype(F32).T.astype(BF16)

    def x_copy(t):
        to = lax.rem(me + t, ns)
        return remote(xsend.at[to], xs.at[me], xsnd.at[t], xrcv.at[me], "section", to)

    def gram_of(i):
        right = s_out[i].reshape(m, width)
        xsend[i] = jnp.dot(part, right, preferred_element_type=F32)

    def gram_stage(t):
        gram_of(lax.rem(me + t, ns))
        x_copy(t).start()

    each(1, ns, gram_stage)
    gram_of(me)

    def gather(t):
        i = lax.rem(me + t, ns)
        remote(xsend.at[i], xs.at[i], xsnd.at[0], xrcv.at[i], "section", i).wait_recv()
        remote(csend.at[i], cs.at[i], csnd.at[i], crcv.at[i], "section", i).wait_recv()

    each(1, ns, gather)
    xt, ct = xsend[me], csend[me]
    for t in range(1, ns):
        i = lax.rem(me + t, ns)
        xt = xt + xs[i]
        ct = ct + cs[i]
    cg[row] = ct
    x_out[row] = xt

    def k_copy(t, slot):
        return remote(
            cg.at[slot], cg.at[slot], ksend.at[t], krecv.at[slot], "row", lax.rem(row + t, nr)
        )

    each(1, nr, lambda t: k_copy(t, row).start())

    deep = w // 2

    def final(h):
        return Line(
            z, nz, c, lambda core, slot: x_out.at[slot * 2 + core, pl.ds(h * deep, deep)],
            lambda q: gup.at[h, q], lambda q: gdown.at[h, q], lambda q: grecv.at[h, q],
            lambda q: hsend.at[h, q], lambda q: hrecv.at[h, q],
        )

    each(0, 2, lambda h: final(h).begin())

    rows = b_out.shape[1]
    start = pl.multiple_of(me * rows, rows)
    b_out[...] = bg[:, pl.ds(start, rows), :]

    each(1, nz, lambda s: each(0, 2, lambda h: final(h).relay(s)))
    each(0, 2, lambda h: final(h).finish())
    per = width // w
    g_out[...] = x_out[pl.ds(me * per, per)].reshape(width, width)
    each(1, nr, lambda t: k_copy(t, lax.rem(row + t, nr)).wait_recv())
    ct = cg[0]
    for k in range(1, nr):
        ct = ct + cg[k]
    c_out[...] = ct

    each(1, nr, lambda t: k_copy(t, row).wait_send())
    first_copy(rsend, rrecv, near(1)).wait_send()
    first_copy(lsend, lrecv, near(-1)).wait_send()
    for d in range(1, far):
        right_copy(d, d + 1 == far).wait_send()
        left_copy(d, d + 1 == far).wait_send()
    each(1, nr, lambda t: probe_copy(t, row).wait_send())

    def drain(j):
        pair_copy(j).wait_send()
        each(1, nz, lambda s: z_copy(j, s, z).wait_send())
        line(j).drain()

    each(0, ns, drain)
    each(1, ns, lambda t: x_copy(t).wait_send())
    each(1, ns, lambda t: c_copy(block(t)).wait_send())
    each(0, 2, lambda h: final(h).drain())


def invert_tile(mat):
    size = mat.shape[0]
    lane = lax.broadcasted_iota(jnp.int32, (size, size), 1)
    sub = lax.broadcasted_iota(jnp.int32, (PAD, size), 0)
    short = lax.broadcasted_iota(jnp.int32, (PAD, size), 1)
    for k in range(0, size, PAD):
        cols = [jnp.broadcast_to(mat[:, k + q:k + q + 1], (size, size)) for q in range(PAD)]
        heads = [col[k:k + PAD] for col in cols]
        rows = jnp.where((short >= k) & (short < k + PAD), 0.0, mat[k:k + PAD])
        rows = rows + jnp.where(short == sub + k, 1.0, 0.0)
        for p in range(PAD):
            scale = 1.0 / heads[p][p:p + 1]
            line = rows[p:p + 1] * scale
            rows = jnp.where(sub == p, line, rows - heads[p] * line)
            for q in range(p + 1, PAD):
                head = heads[q][p:p + 1] * scale
                heads[q] = jnp.where(sub == p, head, heads[q] - heads[p] * head)
        mat = jnp.where((lane >= k) & (lane < k + PAD), 0.0, mat)
        for q in range(PAD):
            mat = mat - cols[q] * rows[q:q + 1]
        parts = [mat[:k], rows, mat[k + PAD:]]
        mat = jnp.concatenate([part for part in parts if part.shape[0]], axis=0)
    return mat


def invert_kernel(x, inv):
    width = inv.shape[0]
    size = min(width, 128)
    inv[...] = x[...]
    column = lax.broadcasted_iota(jnp.int32, (width, width), 1) // size
    eye = (
        lax.broadcasted_iota(jnp.int32, (size, size), 0)
        == lax.broadcasted_iota(jnp.int32, (size, size), 1)
    ).astype(F32)

    def step(b, carry):
        at = pl.ds(pl.multiple_of(b * size, size), size)
        pivot = invert_tile(inv[at, at])
        left = inv[:, at]
        inv[at, at] = eye
        rows = jnp.dot(pivot, inv[at, :], precision=HI, preferred_element_type=F32)
        rest = jnp.where(column == b, 0.0, inv[...])
        inv[...] = rest - jnp.dot(left, rows, precision=HI, preferred_element_type=F32)
        inv[at, :] = rows
        return carry

    lax.fori_loop(0, width // size, step, 0)


def solve_kernel(
    ns, n, x, inv, c0, s_in, p0, b, vec, ortho, coef,
    rbuf, cur, probe_ref, remain_ref, sm, rsend, rrecv, ssend, srecv,
):
    me = lax.axis_index("section")
    m, width = p0.shape[1], c0.shape[1]
    greet((("section", ns),))
    cur[...] = c0[...]

    def r_copy(t, slot):
        return remote(
            rbuf.at[slot], rbuf.at[slot], rsend.at[t], rrecv.at[slot],
            "section", lax.rem(me + t, ns),
        )

    nt = (((1,), (1,)), ((), ()))
    probe_ref[...] = p0[...]
    remain_ref[...] = vec[...]

    def fold(j):
        r = rbuf[j]
        high = r.astype(BF16).astype(F32)
        mid = (r - high).astype(BF16).astype(F32)
        low = r - high - mid
        parts = jnp.concatenate([high, mid, low, jnp.zeros_like(r)], axis=0).astype(BF16)
        moved = lax.dot_general(
            parts, s_in[j].reshape(m, width), nt, preferred_element_type=F32
        )
        probe_ref[...] -= moved[:PAD] + (moved[PAD:2 * PAD] + moved[2 * PAD:3 * PAD])
        taken = lax.dot_general(parts[:2 * PAD], b[j], nt, preferred_element_type=F32)
        remain_ref[...] -= taken[:PAD]

    def chain(j):
        @pl.when(me == j)
        def _():
            rbuf[me] = jnp.dot(cur[...], inv[...], precision=HI, preferred_element_type=F32)
            each(1, ns, lambda t: r_copy(t, me).start())

        pl.when(j > 0)(lambda: fold(j - 1))

        @pl.when(me != j)
        def _():
            remote(rbuf.at[j], rbuf.at[j], rsend.at[0], rrecv.at[j], "section", j).wait_recv()

        @pl.when(me > j)
        def _():
            cur[...] -= jnp.dot(rbuf[j], x[j], precision=HI, preferred_element_type=F32)

    each(0, ns, chain)
    fold(ns - 1)
    probe, remain = probe_ref[...], remain_ref[...]
    small = lax.dot_general(
        probe, probe, (((1,), (1,)), ((), ())), precision=HI, preferred_element_type=F32
    )
    sm[me] = jnp.concatenate([small, jnp.zeros((PAD, 128 - PAD), F32)], axis=1)

    def s_copy(t, slot):
        return remote(
            sm.at[slot], sm.at[slot], ssend.at[t], srecv.at[slot],
            "section", lax.rem(me + t, ns),
        )

    each(1, ns, lambda t: s_copy(t, me).start())
    coef[...] = rbuf[me, :n]
    each(1, ns, lambda t: s_copy(t, lax.rem(me + t, ns)).wait_recv())
    full = sm[0]
    for k in range(1, ns):
        full = full + sm[k]
    low = {}
    rows = []
    for i in range(n):
        for k in range(i + 1):
            value = full[i:i + 1, k:k + 1]
            for q in range(k):
                value = value - low[i, q] * low[k, q]
            low[i, k] = jnp.sqrt(value) if i == k else value / low[k, k]
        line = remain[i:i + 1]
        for k in range(i):
            line = line - low[i, k] * rows[k]
        rows.append(line / low[i, i])
        ortho[i:i + 1, :] = rows[i]
    each(1, ns, lambda t: r_copy(t, me).wait_send())
    each(1, ns, lambda t: s_copy(t, me).wait_send())


def body(ns, nr, omega, basis, vectors):
    dma = pltpu.SemaphoreType.DMA
    n, k = vectors.shape
    m, width = omega.shape[0], basis.shape[1]
    nz = nr // 2
    half = m // 2
    ch = half // nz
    w = ns * width // nr
    rows = k // ns
    vmem = pl.BlockSpec(memory_space=pltpu.VMEM)
    padded = jnp.pad(vectors, ((0, 2 * PAD - n), (0, 0)))
    s_all, x, c0, p0, b, g = pl.pallas_call(
        functools.partial(sketch_kernel, ns, nr),
        out_shape=(
            jax.ShapeDtypeStruct((ns, nr, ch, width), BF16),
            jax.ShapeDtypeStruct((nr, w, width), F32),
            jax.ShapeDtypeStruct((PAD, width), F32),
            jax.ShapeDtypeStruct((PAD, m), F32),
            jax.ShapeDtypeStruct((ns, rows, width), BF16),
            jax.ShapeDtypeStruct((width, width), F32),
        ),
        in_specs=[vmem] * 3,
        out_specs=(vmem,) * 6,
        scratch_shapes=[
            pltpu.VMEM((ns, k, width), BF16),
            pltpu.VMEM((ns, m, width), F32),
            pltpu.VMEM((ns, half, width), F32),
            pltpu.VMEM((ns, nz, ch, width), F32),
            pltpu.VMEM((ns, nz, ch, width), F32),
            pltpu.VMEM((ns, w, width), F32),
            pltpu.VMEM((ns, w, width), F32),
            pltpu.VMEM((ns, PAD, width), F32),
            pltpu.VMEM((ns, PAD, width), F32),
            pltpu.VMEM((nr, PAD, m), F32),
            pltpu.VMEM((max(ch, 128), width), F32),
            pltpu.VMEM((nr, PAD, width), F32),
            dma((ns,)), dma((ns,)), dma((ns,)), dma((ns,)), dma((nr,)), dma((nr,)),
            dma((ns,)), dma((ns,)), dma((ns, nz)), dma((ns, nz)),
            dma((ns, nz)), dma((ns, nz)), dma((ns, nz)), dma((ns, nz)), dma((ns, nz)),
            dma((ns,)), dma((ns,)), dma((ns,)), dma((ns,)),
            dma((2, nz)), dma((2, nz)), dma((2, nz)), dma((2, nz)), dma((2, nz)),
            dma((nr,)), dma((nr,)),
            dma,
        ],
        compiler_params=pltpu.CompilerParams(
            collective_id=0, has_side_effects=True, vmem_limit_bytes=60 * 2**20
        ),
    )(omega, basis, padded)
    x = x.reshape(ns, width, width)
    me = lax.axis_index("section")
    inv = pl.pallas_call(
        invert_kernel,
        out_shape=jax.ShapeDtypeStruct((width, width), F32),
        in_specs=[vmem],
        out_specs=vmem,
        compiler_params=pltpu.CompilerParams(vmem_limit_bytes=32 * 2**20),
    )(g)
    mine = lax.dynamic_slice_in_dim(vectors, me * rows, rows, 1).astype(F32)
    mine = jnp.pad(mine, ((0, PAD - n), (0, 0)))
    return pl.pallas_call(
        functools.partial(solve_kernel, ns, n),
        out_shape=(
            jax.ShapeDtypeStruct((n, rows), F32),
            jax.ShapeDtypeStruct((n, width), F32),
        ),
        in_specs=[vmem] * 7,
        out_specs=(vmem,) * 2,
        scratch_shapes=[
            pltpu.VMEM((ns, PAD, width), F32),
            pltpu.VMEM((PAD, width), F32),
            pltpu.VMEM((PAD, m), F32),
            pltpu.VMEM((PAD, rows), F32),
            pltpu.VMEM((ns, PAD, 128), F32),
            dma((ns,)), dma((ns,)), dma((ns,)), dma((ns,)),
        ],
        compiler_params=pltpu.CompilerParams(
            collective_id=1, has_side_effects=True, vmem_limit_bytes=60 * 2**20
        ),
    )(x, inv, c0, s_all, p0, b, mine)


def solution(mesh):
    return jax.shard_map(
        functools.partial(body, mesh.shape["section"], mesh.shape["row"]),
        mesh=mesh,
        in_specs=(P("section", "row"), P("row", "section"), P(None, "row")),
        out_specs=(P(None, ("row", "section")), P(None, "section")),
        check_vma=False,
    )
```
